16 devices in a mesh: tp: 2 (over z), dp: 8 (over y, x, core).
Axes of the slice: x: 2, y: 2, z: 2, core: 2. Of those that a mesh axis runs over, the one named last changes fastest.
Arguments:
- hidden: bfloat16 [8, 256, 2048], P('dp')
- targets: int32 [8, 256], P('dp')
- weights: float32 [8, 256], P('dp')
- embedding: bfloat16 [49152, 2048], P('tp')
- ln_scale: float32 [2048], replicated
Outputs:
- output 1: float32 [], replicated
- output 2: bfloat16 [8, 256, 2048], P('dp')
- output 3: float32 [49152, 2048], P('tp')
- output 4: float32 [2048], replicated
All inputs are finite; a program needn't handle non-finite values.
Results may differ from the reference program's by a relative error of at most 0.001.
Values sent between devices are 32-bit elements.
A program may use at most 1.25 GiB of HBM per device.

```python
import jax
import jax.numpy as jnp
from jax import lax

BATCH_ROWS = 8
SEQ_LEN = 256
MODEL_DIM = 2048
VOCAB_SIZE = 49152

LN_EPS = 1e-6
Z_WEIGHT = 1e-4
LOGIT_STD = 3.0
ROW_BLOCK = min(SEQ_LEN, 128)
TOKEN_COUNT = BATCH_ROWS * SEQ_LEN
BLOCK_COUNT = TOKEN_COUNT // ROW_BLOCK


def setup_inputs(seed: int = 0) -> dict:
    base_key = jax.random.key(seed)
    route_key, value_key = jax.random.split(base_key, 2)
    key_tgt, key_len = jax.random.split(route_key, 2)
    key_emb, key_noise, key_align, key_wval, key_scale = jax.random.split(value_key, 5)
    emb_gauss = jax.random.normal(key_emb, (VOCAB_SIZE, MODEL_DIM), jnp.float32)
    targets = jax.random.randint(key_tgt, (BATCH_ROWS, SEQ_LEN), 0, VOCAB_SIZE, jnp.int32)
    lengths = jax.random.randint(key_len, (BATCH_ROWS, 1), 1, SEQ_LEN + 1, jnp.int32)
    positions = jnp.arange(SEQ_LEN, dtype=jnp.int32)[None, :]
    keep_mask = (positions < lengths).astype(jnp.float32)
    weights = keep_mask * jax.random.uniform(key_wval, (BATCH_ROWS, SEQ_LEN), jnp.float32, 0.5, 1.5)
    align_amp = jax.random.uniform(key_align, (BATCH_ROWS, SEQ_LEN, 1), jnp.float32, 1.5, 4.5)
    hidden_noise = jax.random.normal(key_noise, (BATCH_ROWS, SEQ_LEN, MODEL_DIM), jnp.float32)
    hidden = hidden_noise + align_amp * (MODEL_DIM ** -0.5) * jnp.take(emb_gauss, targets, axis=0)
    ln_scale = 1.0 + 0.25 * jax.random.normal(key_scale, (MODEL_DIM,), jnp.float32)
    embedding = (emb_gauss * (LOGIT_STD * MODEL_DIM ** -0.5)).astype(jnp.bfloat16)
    return {"hidden": hidden.astype(jnp.bfloat16), "targets": targets, "weights": weights, "embedding": embedding, "ln_scale": ln_scale}


def reference(hidden, targets, weights, embedding, ln_scale):
    total_w = jnp.sum(weights)
    grad_scale = TOKEN_COUNT / total_w
    vocab_ids = jnp.arange(VOCAB_SIZE, dtype=jnp.int32)[None, :]
    h_blocks = hidden.reshape(BLOCK_COUNT, ROW_BLOCK, MODEL_DIM)
    tgt_blocks = targets.reshape(BLOCK_COUNT, ROW_BLOCK)
    w_blocks = weights.reshape(BLOCK_COUNT, ROW_BLOCK)

    def block_step(acc_state, block_in):
        loss_acc, demb_acc, dln_acc = acc_state
        h_blk, tgt_blk, w_blk = block_in
        h_float = h_blk.astype(jnp.float32)
        centered = h_float - jnp.mean(h_float, -1, keepdims=True)
        inv_std = lax.rsqrt(jnp.mean(centered * centered, -1, keepdims=True) + LN_EPS)
        x_hat = centered * inv_std
        h_norm = (x_hat * ln_scale).astype(jnp.bfloat16)
        logits = lax.dot_general(h_norm, embedding, (((1,), (1,)), ((), ())), preferred_element_type=jnp.float32)
        row_max = jnp.max(logits, -1, keepdims=True)
        log_z = row_max + jnp.log(jnp.sum(jnp.exp(logits - row_max), -1, keepdims=True))
        is_target = vocab_ids == tgt_blk[:, None]
        tgt_logit = jnp.sum(jnp.where(is_target, logits, 0.0), -1, keepdims=True)
        loss_tok = log_z - tgt_logit + Z_WEIGHT * log_z * log_z
        loss_acc = loss_acc + jnp.sum(w_blk[:, None] * loss_tok)
        tok_coef = w_blk[:, None] * grad_scale
        soft_prob = jnp.exp(logits - log_z)
        d_logits = ((soft_prob * (1.0 + 2.0 * Z_WEIGHT * log_z) - jnp.where(is_target, 1.0, 0.0)) * tok_coef).astype(jnp.bfloat16)
        d_hn = jnp.dot(d_logits, embedding, preferred_element_type=jnp.float32)
        demb_acc = demb_acc + lax.dot_general(d_logits, h_norm, (((0,), (0,)), ((), ())), preferred_element_type=jnp.float32)
        dln_acc = dln_acc + jnp.sum(d_hn * x_hat, 0)
        d_xhat = d_hn * ln_scale
        d_hblk = inv_std * (d_xhat - jnp.mean(d_xhat, -1, keepdims=True) - x_hat * jnp.mean(d_xhat * x_hat, -1, keepdims=True))
        return (loss_acc, demb_acc, dln_acc), d_hblk.astype(jnp.bfloat16)

    init_state = (jnp.zeros((), jnp.float32), jnp.zeros((VOCAB_SIZE, MODEL_DIM), jnp.float32), jnp.zeros((MODEL_DIM,), jnp.float32))
    final_state, dh_blocks = lax.scan(block_step, init_state, (h_blocks, tgt_blocks, w_blocks))
    loss_sum, d_embedding, d_ln_scale = final_state
    return loss_sum / total_w, dh_blocks.reshape(BATCH_ROWS, SEQ_LEN, MODEL_DIM), d_embedding, d_ln_scale
```

```python
import functools

import jax
import jax.numpy as jnp
from jax import lax
from jax.experimental import pallas as pl
from jax.experimental.pallas import tpu as pltpu
from jax.sharding import PartitionSpec as P

LN_EPS = 1e-6
Z_WEIGHT = 1e-4
MESH = pl.DeviceIdType.MESH
F32 = jnp.float32
BF16 = jnp.bfloat16

S = 256
E = 2048
VT = 24576
VH = VT // 2
NSEQ = 8
NTOK = NSEQ * S
BUCKETS = (1024, 1280, 1536, 2048)

VBA = 1024
NBA = VH // VBA

VB1 = 512
SLOTS = 3
VB2 = 512

NT = (((1,), (1,)), ((), ()))
NN = (((1,), (0,)), ((), ()))


def _flip(dp, k):
    out = dp
    for bit in (1, 2, 4):
        if k & bit:
            out = out + bit * (1 - 2 * lax.rem(dp // bit, 2))
    return out


def _front(x_ref, wy_ref, g_ref, emb_ref, gath_ref, stats_ref, dhn_ref, dln_ref,
           hnf, hnf_sib, xh, hn2, lg, ebuf, dlbuf, acc, dhn_rx, m_s, s_s, t_s, bz, ba, bb, by,
           wy_all, st4, dln_all,
           e_sem, l_sem, row_ss, row_rs, wy_ss, wy_rs, st_ss, st_rs, sq_ss, sq_rs, dl_ss, dl_rs):
    tp = lax.axis_index("tp")
    dp = lax.axis_index("dp")
    core = lax.rem(dp, 2)
    sib = _flip(dp, 1)
    dpx, dpy, dpd = _flip(dp, 2), _flip(dp, 4), _flip(dp, 6)
    here = tp * 2 + core
    bar = pltpu.get_barrier_semaphore()
    for z in (0, 1):
        for k in range(8):
            if z or k:
                pl.semaphore_signal(bar, inc=1, device_id={"tp": tp + z * (1 - 2 * tp), "dp": _flip(dp, k)}, device_id_type=MESH)

    def emb_copy(j):
        row = pl.multiple_of(core * VH + j * VBA, VBA)
        slot = lax.rem(j, 2)
        return pltpu.make_async_copy(emb_ref.at[pl.ds(row, VBA)], ebuf.at[slot], e_sem.at[slot])

    emb_copy(0).start()

    @pl.loop(0, S // 32)
    def _(r):
        rows = pl.ds(pl.multiple_of(r * 32, 32), 32)
        xf = x_ref[rows, :].astype(F32)
        cen = xf - jnp.mean(xf, axis=-1, keepdims=True)
        inv = lax.rsqrt(jnp.mean(cen * cen, axis=-1, keepdims=True) + LN_EPS)
        h = cen * inv
        xh[rows, :] = h
        b = (h * g_ref[...]).astype(BF16)
        hnf[rows, :] = b.astype(F32)
        hn2[pl.ds(pl.multiple_of(core * S + r * 32, 32), 32), :] = b

    pl.semaphore_wait(bar, 15)

    def rcopy(k, src, dst, dev):
        return pltpu.make_async_remote_copy(src_ref=src, dst_ref=dst, send_sem=row_ss.at[k], recv_sem=row_rs.at[k],
                                            device_id={"dp": dev}, device_id_type=MESH)

    H = S // 2
    h0, h1 = pl.ds(0, H), pl.ds(H, H)
    to_sib = rcopy(0, hnf, hnf_sib, sib)
    x0 = rcopy(1, hnf.at[h0], gath_ref.at[dp, h0], dpx)
    x1 = rcopy(2, hnf.at[h1], gath_ref.at[dp, h1], dpx)
    y1 = rcopy(3, hnf.at[h1], gath_ref.at[dp, h1], dpy)
    y0 = rcopy(4, hnf.at[h0], gath_ref.at[dp, h0], dpy)
    d0 = rcopy(5, gath_ref.at[dpx, h0], gath_ref.at[dpx, h0], dpy)
    d1 = rcopy(6, gath_ref.at[dpy, h1], gath_ref.at[dpy, h1], dpx)
    fwd = [rcopy(7 + i, gath_ref.at[q, h], gath_ref.at[q, h], sib)
           for i, (q, h) in enumerate(((dpx, h0), (dpy, h1), (dpx, h1), (dpy, h0), (dpd, h0), (dpd, h1)))]
    dhn_sib = rcopy(13, acc.at[pl.ds(pl.multiple_of((1 - core) * S, S), S)], dhn_rx, sib)

    wy_all[dp] = wy_ref[...]
    wy_cp = [pltpu.make_async_remote_copy(src_ref=wy_ref, dst_ref=wy_all.at[dp], send_sem=wy_ss.at[k], recv_sem=wy_rs.at[k],
                                          device_id={"dp": _flip(dp, k)}, device_id_type=MESH) for k in range(1, 8)]
    to_sib.start()
    for c in wy_cp:
        c.start()
    for c in (x0, y1, x1, y0):
        c.start()
    own_cp = pltpu.make_async_copy(hnf, gath_ref.at[dp], l_sem.at[0])
    own_cp.start()
    to_sib.wait_recv()
    sib_cp = pltpu.make_async_copy(hnf_sib, gath_ref.at[sib], l_sem.at[1])
    sib_cp.start()

    @pl.loop(0, S // 32)
    def _(r):
        rows = pl.ds(pl.multiple_of(r * 32, 32), 32)
        hn2[pl.ds(pl.multiple_of((1 - core) * S + r * 32, 32), 32), :] = hnf_sib[rows, :].astype(BF16)

    for c in wy_cp:
        c.wait()

    def to_cols(rows8):
        full = jnp.concatenate([rows8, jnp.zeros((120, 2 * S), F32)], axis=0)
        return jnp.transpose(full)

    first = dp - core
    wrow = jnp.concatenate([wy_all[first, 0:1], wy_all[first + 1, 0:1]], axis=1)
    yrow = jnp.concatenate([wy_all[first, 1:2], wy_all[first + 1, 1:2]], axis=1)
    cols = to_cols(jnp.broadcast_to(yrow, (8, 2 * S)))
    by[...] = jnp.broadcast_to(cols[:, 0:1], (2 * S, 128)).astype(jnp.int32)
    m_s[...] = jnp.full((2 * S, 128), -1e30, F32)
    s_s[...] = jnp.zeros((2 * S, 128), F32)
    t_s[...] = jnp.zeros((2 * S, 128), F32)
    lane = lax.broadcasted_iota(jnp.int32, (2 * S, 128), 1)
    base = tp * VT + core * VH

    @pl.loop(0, NBA)
    def _(j):
        slot = lax.rem(j, 2)
        emb_copy(j).wait()

        @pl.when(j + 1 < NBA)
        def _():
            emb_copy(j + 1).start()

        l = lax.dot_general(hn2[...], ebuf[slot], NT, preferred_element_type=F32)
        lg[j] = l
        parts = [l[:, c * 128:(c + 1) * 128] for c in range(VBA // 128)]
        mx = m_s[...]
        for p in parts:
            mx = jnp.maximum(mx, p)
        s = s_s[...] * jnp.exp(m_s[...] - mx)
        t = t_s[...]
        yy = by[...] - (base + j * VBA)
        for c, p in enumerate(parts):
            s = s + jnp.exp(p - mx)
            t = t + jnp.where(yy == lane + c * 128, p, 0.0)
        m_s[...] = mx
        s_s[...] = s
        t_s[...] = t

    emb_copy(0).start()
    mx = jnp.max(m_s[...], axis=1, keepdims=True)
    sm = jnp.sum(s_s[...] * jnp.exp(m_s[...] - mx), axis=1, keepdims=True)
    tg = jnp.sum(t_s[...], axis=1, keepdims=True)
    packed = jnp.where(lane == 0, mx, jnp.where(lane == 1, sm, jnp.where(lane == 2, tg, 0.0)))
    st4[here] = jnp.transpose(packed)[0:8, :]
    st_cp = []
    for i, (z, c) in enumerate(((0, 1), (1, 0), (1, 1))):
        st_cp.append(pltpu.make_async_remote_copy(
            src_ref=st4.at[here], dst_ref=st4.at[here], send_sem=st_ss.at[i], recv_sem=st_rs.at[i],
            device_id={"tp": tp + z * (1 - 2 * tp), "dp": _flip(dp, c)}, device_id_type=MESH))
    for c in st_cp:
        c.start()
    x0.wait_recv()
    d0.start()
    fwd[0].start()
    y1.wait_recv()
    d1.start()
    fwd[1].start()
    total_w = jnp.sum(jnp.concatenate([wy_all[q, 0:1] for q in range(NSEQ)], axis=0))
    for c in st_cp:
        c.wait()
    ms = [st4[q, 0:1] for q in range(4)]
    mg = jnp.maximum(jnp.maximum(ms[0], ms[1]), jnp.maximum(ms[2], ms[3]))
    sg = jnp.zeros_like(mg)
    tgr = jnp.zeros_like(mg)
    for q in range(4):
        sg = sg + st4[q, 1:2] * jnp.exp(ms[q] - mg)
        tgr = tgr + st4[q, 2:3]
    logz = mg + jnp.log(sg)
    scale = jnp.full((1, 2 * S), float(NTOK), F32) / total_w
    coef_b = wrow * scale
    coef_a = coef_b * (1.0 + 2.0 * Z_WEIGHT * logz)
    sub = lax.broadcasted_iota(jnp.int32, (8, 2 * S), 0)
    rows8 = jnp.where(sub == 0, wrow, jnp.where(sub == 1, yrow, jnp.where(sub == 2, logz, jnp.where(
        sub == 3, tgr, jnp.where(sub == 4, coef_a, jnp.where(sub == 5, coef_b, 0.0))))))
    stats_ref[dp] = jnp.where(core == 0, rows8[:, :S], rows8[:, S:])
    sq_cp = [pltpu.make_async_remote_copy(src_ref=stats_ref.at[dp], dst_ref=stats_ref.at[dp], send_sem=sq_ss.at[k],
                                          recv_sem=sq_rs.at[k], device_id={"dp": _flip(dp, k)}, device_id_type=MESH)
             for k in range(1, 8)]
    for c in sq_cp:
        c.start()
    cols = to_cols(rows8)
    bz[...] = jnp.broadcast_to(cols[:, 2:3], (2 * S, 128))
    ba[...] = jnp.broadcast_to(cols[:, 4:5], (2 * S, 128))
    bb[...] = jnp.broadcast_to(cols[:, 5:6], (2 * S, 128))
    acc[...] = jnp.zeros((2 * S, E), F32)

    @pl.loop(0, NBA)
    def _(j):
        slot = lax.rem(j, 2)
        emb_copy(j).wait()

        @pl.when(j + 1 < NBA)
        def _():
            emb_copy(j + 1).start()

        yy = by[...] - (base + j * VBA)
        z, a, b = bz[...], ba[...], bb[...]
        for c in range(VBA // 128):
            p = jnp.exp(lg[j, :, c * 128:(c + 1) * 128] - z) * a
            dlbuf[:, c * 128:(c + 1) * 128] = (p - jnp.where(yy == lane + c * 128, b, 0.0)).astype(BF16)
        acc[...] += lax.dot_general(dlbuf[...], ebuf[slot], NN, preferred_element_type=F32)

    dhn_sib.start()
    x1.wait_recv()
    fwd[2].start()
    y0.wait_recv()
    fwd[3].start()
    dhn_sib.wait_recv()

    dln = jnp.zeros((8, E), F32)
    dhn_ref[...] = acc[pl.ds(pl.multiple_of(core * S, S), S), :] + dhn_rx[...]
    for r in range(S // 8):
        dln = dln + dhn_ref[r * 8:(r + 1) * 8, :] * xh[r * 8:(r + 1) * 8, :]
    me16 = tp * 8 + dp
    dln_all[me16] = jnp.sum(dln, axis=0, keepdims=True)
    dln_cp = []
    for z in (0, 1):
        for k in range(8):
            if z or k:
                i = z * 8 + k
                dln_cp.append(pltpu.make_async_remote_copy(
                    src_ref=dln_all.at[me16], dst_ref=dln_all.at[me16], send_sem=dl_ss.at[i], recv_sem=dl_rs.at[i],
                    device_id={"tp": tp + z * (1 - 2 * tp), "dp": _flip(dp, k)}, device_id_type=MESH))
    for c in dln_cp:
        c.start()
    d0.wait_recv()
    fwd[4].start()
    d1.wait_recv()
    fwd[5].start()
    for c in sq_cp + dln_cp:
        c.wait()
    out = dln_all[0]
    for q in range(1, 16):
        out = out + dln_all[q]
    dln_ref[...] = out
    own_cp.wait()
    sib_cp.wait()
    for c in (to_sib, x0, x1, y0, y1, d0, d1, dhn_sib):
        c.wait_send()
    for c in fwd:
        c.wait()


def front(x, wy, g, emb):
    vm = pl.BlockSpec(memory_space=pltpu.VMEM)
    hbm = pl.BlockSpec(memory_space=pl.ANY)
    dma = pltpu.SemaphoreType.DMA
    return pl.pallas_call(
        _front,
        out_shape=(jax.ShapeDtypeStruct((NSEQ, S, E), F32), jax.ShapeDtypeStruct((NSEQ, 8, S), F32),
                   jax.ShapeDtypeStruct((S, E), F32), jax.ShapeDtypeStruct((1, E), F32)),
        in_specs=[vm, vm, vm, hbm], out_specs=(hbm, vm, vm, vm),
        scratch_shapes=[
            pltpu.VMEM((S, E), F32), pltpu.VMEM((S, E), F32), pltpu.VMEM((S, E), F32), pltpu.VMEM((2 * S, E), BF16),
            pltpu.VMEM((NBA, 2 * S, VBA), F32), pltpu.VMEM((2, VBA, E), BF16), pltpu.VMEM((2 * S, VBA), BF16),
            pltpu.VMEM((2 * S, E), F32), pltpu.VMEM((S, E), F32),
            pltpu.VMEM((2 * S, 128), F32), pltpu.VMEM((2 * S, 128), F32), pltpu.VMEM((2 * S, 128), F32),
            pltpu.VMEM((2 * S, 128), F32), pltpu.VMEM((2 * S, 128), F32), pltpu.VMEM((2 * S, 128), F32),
            pltpu.VMEM((2 * S, 128), jnp.int32),
            pltpu.VMEM((NSEQ, 8, S), F32), pltpu.VMEM((4, 8, 2 * S), F32), pltpu.VMEM((16, 1, E), F32),
            dma((2,)), dma((2,)), dma((14,)), dma((14,)), dma((8,)), dma((8,)), dma((3,)), dma((3,)),
            dma((8,)), dma((8,)), dma((16,)), dma((16,)),
        ],
        compiler_params=pltpu.CompilerParams(collective_id=0, has_side_effects=True, vmem_limit_bytes=64 * 1024 * 1024 - 65536),
        cost_estimate=pl.CostEstimate(flops=2 * 2 * 2 * S * VH * E, bytes_accessed=2 * VH * E * 2, transcendentals=0),
        name="front",
    )(x, wy, g, emb)


def _pack(stats_ref, gath_ref, hc_ref, rows_ref, gbuf, dest, off_s, g_sem):
    ob = pl.program_id(0)

    def g_copy(s):
        return pltpu.make_async_copy(gath_ref.at[s], gbuf.at[s], g_sem.at[s])

    @pl.when(ob == 0)
    def _():
        for s in range(NSEQ):
            g_copy(s).start()
        act = (stats_ref[:, 0, :] > 0.0)
        af = jnp.where(act, 1.0, 0.0)
        i0 = lax.broadcasted_iota(jnp.int32, (S, S), 0)
        i1 = lax.broadcasted_iota(jnp.int32, (S, S), 1)
        upper = jnp.where(i0 < i1, 1.0, 0.0).astype(BF16)
        pos = jnp.dot(af.astype(BF16), upper, preferred_element_type=F32).astype(jnp.int32)
        off = jnp.int32(0)
        for s in range(NSEQ):
            off_s[s] = off
            dest[s] = jnp.broadcast_to(jnp.where(act[s:s + 1], pos[s:s + 1] + off, -1), (8, S))
            off = off + jnp.sum(af[s:s + 1]).astype(jnp.int32)
        off_s[NSEQ] = off
        for s in range(NSEQ):
            g_copy(s).wait()

    hacc = gbuf.at[NSEQ]
    hacc[...] = jnp.zeros((S, E), F32)
    racc = gbuf.at[NSEQ + 1, :, 0:128]
    racc[...] = jnp.zeros((S, 128), F32)
    r = lax.broadcasted_iota(jnp.int32, (S, S), 0) + ob * S
    lane = lax.broadcasted_iota(jnp.int32, (S, 128), 1)
    for s in range(NSEQ):
        @pl.when((off_s[s] < (ob + 1) * S) & (off_s[s + 1] > ob * S))
        def _(s=s):
            hit = dest[s, 0:1] == r
            hacc[...] += jnp.dot(jnp.where(hit, 1.0, 0.0).astype(BF16), gbuf[s].astype(BF16), preferred_element_type=F32)
            add = jnp.zeros((S, 128), F32)
            for i, k in enumerate((1, 2, 4, 5)):
                v = jnp.sum(jnp.where(hit, stats_ref[s, k:k + 1], 0.0), axis=1, keepdims=True)
                add = jnp.where(lane == i, v, add)
            racc[...] += add
    hc_ref[...] = hacc[...].astype(BF16)
    rows_ref[...] = jnp.transpose(racc[...])[0:8, :]


def pack(stats, gath):
    return pl.pallas_call(
        _pack, grid=(NTOK // S,),
        out_shape=(jax.ShapeDtypeStruct((NTOK, E), BF16), jax.ShapeDtypeStruct((8, NTOK), F32)),
        in_specs=[pl.BlockSpec((NSEQ, 8, S), lambda i: (0, 0, 0)), pl.BlockSpec(memory_space=pl.ANY)],
        out_specs=(pl.BlockSpec((S, E), lambda i: (i, 0)), pl.BlockSpec((8, S), lambda i: (0, i))),
        scratch_shapes=[pltpu.VMEM((NSEQ + 2, S, E), F32), pltpu.VMEM((NSEQ, 8, S), jnp.int32), pltpu.SMEM((NSEQ + 1,), jnp.int32),
                        pltpu.SemaphoreType.DMA((NSEQ,))],
        compiler_params=pltpu.CompilerParams(dimension_semantics=("arbitrary",), vmem_limit_bytes=60 * 1024 * 1024),
        name="pack",
    )(stats, gath)


def _dlogits(n, hc_ref, rows_ref, emb_ref, dl_ref, hc, ebuf, sbuf, h_sem, e_sem, w_sem, ss, rs):
    tp = lax.axis_index("tp")
    dp = lax.axis_index("dp")
    core = lax.rem(dp, 2)
    sib = _flip(dp, 1)
    nblk = VH // VB1
    steps = nblk // 6 * 7
    bar = pltpu.get_barrier_semaphore()
    pl.semaphore_signal(bar, inc=1, device_id={"dp": sib}, device_id_type=MESH)

    def row_of(i):
        q, k = i // 7, lax.rem(i, 7)
        extra = k // 6
        half = core + extra * (1 - 2 * core)
        return pl.multiple_of(half * VH + (q * 6 + k - extra) * VB1, VB1)

    def emb_copy(i):
        slot = lax.rem(i, 2)
        return pltpu.make_async_copy(emb_ref.at[pl.ds(row_of(i), VB1)], ebuf.at[slot], e_sem.at[slot])

    def out_copy(i):
        slot = lax.rem(i, SLOTS)
        return pltpu.make_async_copy(sbuf.at[slot], dl_ref.at[pl.ds(row_of(i), VB1)], w_sem.at[slot])

    def send_copy(i):
        slot = lax.rem(i, SLOTS)
        rows = pl.ds(row_of(i), VB1)
        return pltpu.make_async_remote_copy(src_ref=sbuf.at[slot], dst_ref=dl_ref.at[rows], send_sem=ss.at[slot],
                                            recv_sem=rs.at[i // 7 * 5 + lax.rem(i, 7)], device_id={"dp": sib}, device_id_type=MESH)

    h_copy = pltpu.make_async_copy(hc_ref.at[pl.ds(0, n)], hc, h_sem)
    h_copy.start()
    emb_copy(0).start()
    h_copy.wait()
    pl.semaphore_wait(bar, 1)
    logz, coef_a, coef_b = rows_ref[1:2, :n], rows_ref[2:3, :n], rows_ref[3:4, :n]
    sub = lax.broadcasted_iota(jnp.int32, (VB1, n), 0)

    @pl.loop(0, steps)
    def _(i):
        slot = lax.rem(i, SLOTS)
        emb_copy(i).wait()

        @pl.when(i + 1 < steps)
        def _():
            emb_copy(i + 1).start()

        @pl.when(i >= SLOTS)
        def _():
            out_copy(i - SLOTS).wait()

            @pl.when(lax.rem(i - SLOTS, 7) < 5)
            def _():
                send_copy(i - SLOTS).wait_send()

        yy = rows_ref[0:1, :n].astype(jnp.int32) - (tp * VT + row_of(i))
        l = lax.dot_general(ebuf[lax.rem(i, 2)], hc[...], NT, preferred_element_type=F32)
        p = jnp.exp(l - logz) * coef_a
        sbuf[slot] = p - jnp.where(sub == yy, coef_b, 0.0)
        out_copy(i).start()

        @pl.when(lax.rem(i, 7) < 5)
        def _():
            send_copy(i).start()

    for i in range(steps - SLOTS, steps):
        out_copy(i).wait()
        if i % 7 < 5:
            send_copy(i).wait_send()

    @pl.loop(0, nblk // 6 * 5)
    def _(i):
        send_copy(i // 5 * 7 + lax.rem(i, 5)).wait_recv()


def dlogits(n, cid, hc, rows, emb):
    dma = pltpu.SemaphoreType.DMA
    return pl.pallas_call(
        functools.partial(_dlogits, n),
        out_shape=jax.ShapeDtypeStruct((VT, n), F32),
        in_specs=[pl.BlockSpec(memory_space=pl.ANY), pl.BlockSpec(memory_space=pltpu.VMEM), pl.BlockSpec(memory_space=pl.ANY)],
        out_specs=pl.BlockSpec(memory_space=pl.ANY),
        scratch_shapes=[pltpu.VMEM((n, E), BF16), pltpu.VMEM((2, VB1, E), BF16), pltpu.VMEM((SLOTS, VB1, n), F32),
                        dma, dma((2,)), dma((SLOTS,)), dma((SLOTS,)), dma((VH // VB1 // 6 * 5,))],
        compiler_params=pltpu.CompilerParams(collective_id=cid, has_side_effects=True, vmem_limit_bytes=60 * 1024 * 1024),
        cost_estimate=pl.CostEstimate(flops=2 * VH * n * E, bytes_accessed=VH * E * 2 + 2 * VH * n * 4, transcendentals=0),
        name=f"dlogits{n}",
    )(hc, rows, emb)


def _demb(dl_ref, hc_ref, out_ref):
    out_ref[...] = jnp.dot(dl_ref[...].astype(BF16), hc_ref[...], preferred_element_type=F32)


def demb(n, dl, hc):
    return pl.pallas_call(
        _demb, grid=(VT // VB2,),
        out_shape=jax.ShapeDtypeStruct((VT, E), F32),
        in_specs=[pl.BlockSpec((VB2, n), lambda i: (i, 0)), pl.BlockSpec((n, E), lambda i: (0, 0), pipeline_mode=pl.Buffered(1))],
        out_specs=pl.BlockSpec((VB2, E), lambda i: (i, 0)),
        compiler_params=pltpu.CompilerParams(dimension_semantics=("arbitrary",), vmem_limit_bytes=60 * 1024 * 1024),
        cost_estimate=pl.CostEstimate(flops=2 * VT * n * E, bytes_accessed=VT * E * 4 + VT * n * 4, transcendentals=0),
        name=f"demb{n}",
    )(dl, hc)


def solution(mesh):
    def local_step(hidden, targets, weights, embedding, ln_scale):
        x = hidden[0]
        g = ln_scale[None, :]
        wy = jnp.concatenate([weights, targets.astype(F32), jnp.zeros((6, S), F32)], axis=0)
        gath, stats, dhn, dln = front(x, wy, g, embedding)
        dhn_other = lax.ppermute(dhn, "tp", [(0, 1), (1, 0)])
        hc, rows = pack(stats, gath)
        w_all = stats[:, 0, :]
        count = jnp.sum((w_all > 0.0).astype(jnp.int32))
        which = sum((count > b).astype(jnp.int32) for b in BUCKETS[:-1])

        def branch(i, n):
            def run(hc, rows, emb):
                return demb(n, dlogits(n, 1 + i, hc, rows, emb), hc)
            return run

        d_emb = lax.switch(which, [branch(i, n) for i, n in enumerate(BUCKETS)], hc, rows, embedding)
        log_z, tgt = stats[:, 2, :], stats[:, 3, :]
        mean_loss = jnp.sum(w_all * (log_z - tgt + Z_WEIGHT * log_z * log_z)) / jnp.sum(w_all)

        h_float = x.astype(F32)
        centered = h_float - jnp.mean(h_float, -1, keepdims=True)
        inv_std = lax.rsqrt(jnp.mean(centered * centered, -1, keepdims=True) + LN_EPS)
        x_hat = centered * inv_std
        a = (dhn + dhn_other) * ln_scale
        d_hidden = inv_std * (a - jnp.mean(a, -1, keepdims=True) - x_hat * jnp.mean(a * x_hat, -1, keepdims=True))
        return mean_loss, d_hidden.astype(BF16)[None], d_emb, dln[0]

    return jax.shard_map(local_step, mesh=mesh,
                         in_specs=(P("dp", None, None), P("dp", None), P("dp", None), P("tp", None), P(None)),
                         out_specs=(P(), P("dp", None, None), P("tp", None), P(None)), check_vma=False)
```

```python
import functools

import jax
import jax.numpy as jnp
from jax import lax
from jax.experimental import pallas as pl
from jax.experimental.pallas import tpu as pltpu
from jax.sharding import PartitionSpec as P

LN_EPS = 1e-6
Z_WEIGHT = 1e-4
LOG2E = 1.4426950408889634
LN2 = 0.6931471805599453
MESH = pl.DeviceIdType.MESH
F32 = jnp.float32
BF16 = jnp.bfloat16

S = 256
E = 2048
S2 = S + S
LANE = 128
VT = 24576
VH = VT // 2
NSEQ = 8
NTOK = NSEQ * S
BUCKETS = (768, 1024, 1280, 1536, 2048)
ALIGN = 8

VBA = 2048
NBA = VH // VBA
LNR = 64

VB1 = 512
SLOTS = 5
GROUP, SENT, TURN = 12, 11, 13
VB2 = 512

NT = (((1,), (1,)), ((), ()))
NN = (((1,), (0,)), ((), ()))


def _flip(dp, k):
    out = dp
    for bit in (1, 2, 4):
        if k & bit:
            out = out + bit * (1 - 2 * lax.rem(dp // bit, 2))
    return out


def _dev(tp, dp, z, k):
    return {"tp": tp + z * (1 - 2 * tp), "dp": _flip(dp, k)}


def _remote(src, dst, ss, rs, dev):
    return pltpu.make_async_remote_copy(src_ref=src, dst_ref=dst, send_sem=ss, recv_sem=rs, device_id=dev, device_id_type=MESH)


def _to_cols(rows8):
    return jnp.transpose(jnp.concatenate([rows8, jnp.zeros((120, rows8.shape[1]), F32)], axis=0))


def _places(w):
    i0 = lax.broadcasted_iota(jnp.int32, (S, S), 0)
    i1 = lax.broadcasted_iota(jnp.int32, (S, S), 1)
    flags = jnp.broadcast_to(jnp.where(w > 0.0, 1.0, 0.0), (8, S)).astype(BF16)
    pos = jnp.dot(flags, jnp.where(i0 < i1, 1.0, 0.0).astype(BF16), preferred_element_type=F32)[0:1]
    return jnp.where(w > 0.0, pos, -1.0)


def _norm(xf):
    cen = xf - jnp.mean(xf, axis=-1, keepdims=True)
    inv = lax.rsqrt(jnp.mean(cen * cen, axis=-1, keepdims=True) + LN_EPS)
    return cen * inv, inv


def _front(x_ref, w_ref, y_ref, g_ref, emb_ref, gath_ref, stats_ref, own_ref, sib_ref, dln_ref, cnt_ref, which_ref,
           hnf, xh, hn2, lg, ebuf, dlbuf, acc, m_s, s_s, t_s, bz, bb, by, wyc, wy_all, st4,
           e_sem, l_sem, row_ss, row_rs, wy_ss, wy_rs, st_ss, st_rs, sq_ss, sq_rs):
    tp = lax.axis_index("tp")
    dp = lax.axis_index("dp")
    core = lax.rem(dp, 2)
    sib = _flip(dp, 1)
    dpx, dpy, dpd = _flip(dp, 2), _flip(dp, 4), _flip(dp, 6)
    here = tp * 2 + core
    bar = pltpu.get_barrier_semaphore()
    for k in range(1, 8):
        pl.semaphore_signal(bar, inc=1, device_id=_dev(tp, dp, 0, k), device_id_type=MESH)
    for k in (0, 1):
        pl.semaphore_signal(bar, inc=1, device_id=_dev(tp, dp, 1, k), device_id_type=MESH)

    def emb_copy(j):
        row = pl.multiple_of(core * VH + j * VBA, VBA)
        slot = lax.rem(j, 2)
        return pltpu.make_async_copy(emb_ref.at[pl.ds(row, VBA)], ebuf.at[slot], e_sem.at[slot])

    emb_copy(0).start()
    i0 = lax.broadcasted_iota(jnp.int32, (S, S), 0)
    hit = i0 == _places(w_ref[...]).astype(jnp.int32)
    xc, xc_sib = acc.at[0:S], acc.at[S:S2]
    xc[...] = jnp.dot(jnp.where(hit, 1.0, 0.0).astype(BF16), x_ref[...], preferred_element_type=F32)
    wc = jnp.sum(jnp.where(hit, w_ref[...], 0.0), axis=1, keepdims=True)
    yc = jnp.sum(jnp.where(hit, y_ref[...].astype(F32), 0.0), axis=1, keepdims=True)
    ln = lax.broadcasted_iota(jnp.int32, (S, LANE), 1)
    wyc[...] = jnp.transpose(jnp.where(ln == 0, wc, jnp.where(ln == 1, yc, 0.0)))[0:8, :]
    wy_all[dp] = wyc[...]

    def layer_norm(src, half, keep):
        @pl.loop(0, S // LNR)
        def _(r):
            rows = pl.ds(pl.multiple_of(r * LNR, LNR), LNR)
            at = pl.ds(pl.multiple_of(half * S + r * LNR, LNR), LNR)
            h, _ = _norm(src[rows, :])
            xh[at, :] = h
            b = (h * g_ref[...]).astype(BF16)
            hn2[at, :] = b
            if keep:
                hnf[rows, :] = b.astype(F32)

    layer_norm(xc, core, True)
    pl.semaphore_wait(bar, 9)

    def rcopy(k, src, dst, dev):
        return _remote(src, dst, row_ss.at[k], row_rs.at[k], dev)

    Q = S // 4

    def quarter(k, part=0, parts=1):
        q = k + tp * (3 - 2 * k)
        return pl.ds(pl.multiple_of(q * Q + part * (Q // parts), 8), Q // parts)

    to_x, to_y, to_sib, to_z = _dev(tp, dp, 0, 2), _dev(tp, dp, 0, 4), _dev(tp, dp, 0, 1), _dev(tp, dp, 1, 0)
    x_cp = rcopy(0, xc, xc_sib, to_sib)

    def onward(k, q, rows, dev):
        return rcopy(k, gath_ref.at[q, rows], gath_ref.at[q, rows], dev)

    ex = [rcopy(1 + k, hnf.at[quarter(k)], gath_ref.at[dp, quarter(k)], to_x) for k in range(3)]
    ey = [rcopy(4 + k, hnf.at[quarter(k)], gath_ref.at[dp, quarter(k)], to_y) for k in range(3)]
    d0, d1 = onward(7, dpx, quarter(0), to_y), onward(8, dpy, quarter(1), to_x)
    d2, d3 = onward(9, dpx, quarter(2, 0, 2), to_y), onward(10, dpy, quarter(2, 1, 2), to_x)
    zx, zy, zd = (onward(11 + i, q, quarter(0), to_z) for i, q in enumerate((dpx, dpy, dpd)))
    fx, fy, fd = ([onward(14 + 4 * i + k, q, quarter(k), to_sib) for k in range(4)] for i, q in enumerate((dpx, dpy, dpd)))
    f_own = onward(26, dp, pl.ds(0, S), to_sib)
    wy_cp = [_remote(wyc, wy_all.at[dp], wy_ss.at[k], wy_rs.at[k], _dev(tp, dp, 0, k)) for k in range(1, 8)]
    x_cp.start()
    for c in wy_cp:
        c.start()

    for c in (ex[0], ey[1], ex[1], ey[0]):
        c.start()
    own_cp = pltpu.make_async_copy(hnf, gath_ref.at[dp], l_sem.at[0])
    own_cp.start()
    for c in wy_cp:
        c.wait()
    first = dp - core
    wrow = jnp.concatenate([wy_all[first, 0:1], wy_all[first + 1, 0:1]], axis=1)
    yrow = jnp.concatenate([wy_all[first, 1:2], wy_all[first + 1, 1:2]], axis=1)
    cols = _to_cols(jnp.broadcast_to(yrow, (8, S2)))
    by[...] = jnp.broadcast_to(cols[:, 0:1], (S2, LANE)).astype(jnp.int32)
    m_s[...] = jnp.full((S2, LANE), -1e30, F32)
    s_s[...] = jnp.zeros((S2, LANE), F32)
    t_s[...] = jnp.zeros((S2, LANE), F32)
    lane = lax.broadcasted_iota(jnp.int32, (S2, LANE), 1)
    base = tp * VT + core * VH
    x_cp.wait_recv()
    layer_norm(xc_sib, 1 - core, False)
    x_cp.wait_send()
    acc[...] = jnp.zeros((S2, E), F32)

    @pl.loop(0, NBA)
    def _(j):
        slot = lax.rem(j, 2)
        emb_copy(j).wait()

        @pl.when(j + 1 < NBA)
        def _():
            emb_copy(j + 1).start()

        @pl.when(j == 2)
        def _():
            ex[0].wait_recv()
            for c in (d0, zx):
                c.start()
            ey[1].wait_recv()
            for c in (d1, ex[2], ey[2], fx[0], fy[1]):
                c.start()

        @pl.when(j == 4)
        def _():
            ey[0].wait_recv()
            for c in (zy, fy[0]):
                c.start()
            ex[1].wait_recv()
            fx[1].start()

        l = lax.dot_general(hn2[...], ebuf[slot], NT, preferred_element_type=F32) * LOG2E
        lg[j] = l
        parts = [l[:, c * LANE:(c + 1) * LANE] for c in range(VBA // LANE)]
        mx = m_s[...]
        for p in parts:
            mx = jnp.maximum(mx, p)
        s = s_s[...] * jnp.exp2(m_s[...] - mx)
        t = t_s[...]
        yy = by[...] - (base + j * VBA)
        for c, p in enumerate(parts):
            s = s + jnp.exp2(p - mx)
            t = jnp.where(yy == lane + c * LANE, p, t)
        m_s[...] = mx
        s_s[...] = s
        t_s[...] = t

    emb_copy(0).start()
    mx = jnp.max(m_s[...], axis=1, keepdims=True)
    sm = jnp.sum(s_s[...] * jnp.exp2(m_s[...] - mx), axis=1, keepdims=True)
    tg = jnp.sum(t_s[...], axis=1, keepdims=True)
    packed = jnp.where(lane == 0, mx, jnp.where(lane == 1, sm, jnp.where(lane == 2, tg, 0.0)))
    st4[here] = jnp.transpose(packed)[0:8, :]
    st_cp = [_remote(st4.at[here], st4.at[here], st_ss.at[i], st_rs.at[i], _dev(tp, dp, z, k))
             for i, (z, k) in enumerate(((0, 1), (1, 0), (1, 1)))]
    for c in st_cp:
        c.start()
    w8 = jnp.concatenate([wy_all[q, 0:1] for q in range(NSEQ)], axis=0)
    total = jnp.sum(w8)
    start = jnp.int32(0)
    for q in range(NSEQ):
        cnt = jnp.sum(jnp.where(w8[q:q + 1] > 0.0, 1.0, 0.0)).astype(jnp.int32)
        cnt_ref[q] = cnt
        cnt_ref[NSEQ + q] = start
        start = start + (cnt + ALIGN - 1) // ALIGN * ALIGN
    which = sum((start > t).astype(jnp.int32) for t in BUCKETS[:-1])
    which_ref[0] = which
    cnt_ref[2 * NSEQ] = BUCKETS[0] // S + sum((which > i).astype(jnp.int32) * ((BUCKETS[i + 1] - BUCKETS[i]) // S) for i in range(len(BUCKETS) - 1))
    own_cp.wait()
    f_own.start()
    d0.wait_recv()
    for c in (zd, fd[0]):
        c.start()
    d1.wait_recv()
    fd[1].start()
    for c in st_cp:
        c.wait()
    ms = [st4[q, 0:1] for q in range(4)]
    mg = jnp.maximum(jnp.maximum(ms[0], ms[1]), jnp.maximum(ms[2], ms[3]))
    sg = jnp.zeros_like(mg)
    tgr = jnp.zeros_like(mg)
    for q in range(4):
        sg = sg + st4[q, 1:2] * jnp.exp2(ms[q] - mg)
        tgr = tgr + st4[q, 2:3]
    logz = (mg + jnp.log2(sg)) * LN2
    tgr = tgr * LN2
    coef_b = wrow * (jnp.full((1, S2), float(NTOK), F32) / total)
    coef_a = coef_b * (1.0 + 2.0 * Z_WEIGHT * logz)
    shift = jnp.where(coef_a > 0.0, mg + jnp.log2(sg) - jnp.log2(coef_a), 1e30)
    sub = lax.broadcasted_iota(jnp.int32, (8, S2), 0)
    rows8 = jnp.where(sub == 0, yrow, jnp.where(sub == 1, logz, jnp.where(sub == 2, shift, jnp.where(
        sub == 3, coef_b, jnp.where(sub == 4, tgr, jnp.where(sub == 5, wrow, total))))))
    stats_ref[dp] = jnp.where(core == 0, rows8[:, :S], rows8[:, S:])
    sq_cp = [_remote(stats_ref.at[dp], stats_ref.at[dp], sq_ss.at[k], sq_rs.at[k], _dev(tp, dp, 0, k)) for k in range(1, 8)]
    for c in sq_cp:
        c.start()
    cols = _to_cols(rows8)
    bz[...] = jnp.broadcast_to(cols[:, 2:3], (S2, LANE))
    bb[...] = jnp.broadcast_to(cols[:, 3:4], (S2, LANE))

    @pl.loop(0, NBA)
    def _(j):
        slot = lax.rem(j, 2)
        emb_copy(j).wait()

        @pl.when(j + 1 < NBA)
        def _():
            emb_copy(j + 1).start()

        @pl.when(j == NBA // 3)
        def _():
            ex[2].wait_recv()
            for c in (d2, fx[2]):
                c.start()
            ey[2].wait_recv()
            for c in (d3, fy[2]):
                c.start()
            zx.wait_recv()
            fx[3].start()
            zy.wait_recv()
            fy[3].start()

        @pl.when(j == NBA - 1)
        def _():
            d2.wait_recv()
            d3.wait_recv()
            fd[2].start()

        yy = by[...] - (base + j * VBA)
        z, b = bz[...], bb[...]
        for c in range(VBA // LANE):
            p = jnp.exp2(lg[j, :, c * LANE:(c + 1) * LANE] - z)
            dlbuf[:, c * LANE:(c + 1) * LANE] = jnp.where(yy == lane + c * LANE, p - b, p).astype(BF16)
        acc[...] += lax.dot_general(dlbuf[...], ebuf[slot], NN, preferred_element_type=F32)

    own_out = pltpu.make_async_copy(acc.at[pl.ds(pl.multiple_of(core * S, S), S)], own_ref, l_sem.at[0])
    sib_out = pltpu.make_async_copy(acc.at[pl.ds(pl.multiple_of((1 - core) * S, S), S)], sib_ref, l_sem.at[1])
    own_out.start()
    sib_out.start()
    zd.wait_recv()
    fd[3].start()
    dln = jnp.zeros((8, E), F32)
    for q in range(S2 // 8):
        dln = dln + acc[q * 8:(q + 1) * 8, :] * xh[q * 8:(q + 1) * 8, :]
    dln_ref[...] = jnp.sum(dln, axis=0, keepdims=True)
    for c in sq_cp:
        c.wait()
    own_out.wait()
    sib_out.wait()
    for c in ex + ey + [d0, d1, d2, d3, zx, zy, zd]:
        c.wait_send()
    for c in fx + fy + fd + [f_own]:
        c.wait()


def front(x, w, y, g, emb):
    vm = pl.BlockSpec(memory_space=pltpu.VMEM)
    hbm = pl.BlockSpec(memory_space=pl.ANY)
    dma = pltpu.SemaphoreType.DMA
    sm = pl.BlockSpec(memory_space=pltpu.SMEM)
    tile = pltpu.VMEM((S2, LANE), F32)
    seq = jax.ShapeDtypeStruct((S, E), F32)
    return pl.pallas_call(
        _front,
        out_shape=(jax.ShapeDtypeStruct((NSEQ, S, E), F32), jax.ShapeDtypeStruct((NSEQ, 8, S), F32), seq, seq,
                   jax.ShapeDtypeStruct((1, E), F32), jax.ShapeDtypeStruct((32,), jnp.int32), jax.ShapeDtypeStruct((1,), jnp.int32)),
        in_specs=[vm, vm, vm, vm, hbm], out_specs=(hbm, vm, hbm, hbm, vm, sm, sm),
        scratch_shapes=[
            pltpu.VMEM((S, E), F32), pltpu.VMEM((S2, E), F32), pltpu.VMEM((S2, E), BF16),
            pltpu.VMEM((NBA, S2, VBA), F32), pltpu.VMEM((2, VBA, E), BF16), pltpu.VMEM((S2, VBA), BF16),
            pltpu.VMEM((S2, E), F32), tile, tile, tile, tile, tile, pltpu.VMEM((S2, LANE), jnp.int32),
            pltpu.VMEM((8, S), F32), pltpu.VMEM((NSEQ, 8, S), F32), pltpu.VMEM((4, 8, S2), F32),
            dma((2,)), dma((2,)), dma((27,)), dma((27,)), dma((8,)), dma((8,)), dma((3,)), dma((3,)), dma((8,)), dma((8,)),
        ],
        compiler_params=pltpu.CompilerParams(collective_id=0, has_side_effects=True, vmem_limit_bytes=67043328),
        cost_estimate=pl.CostEstimate(flops=2 * 2 * S2 * VH * E, bytes_accessed=2 * VH * E * 2, transcendentals=0),
        name="front",
    )(x, w, y, g, emb)


def _pack(cnt_ref, stats_ref, gath_ref, hc_ref, rows_ref, loss_ref, stage, hbuf, g_sem, h_sem):
    def copy(s, k, rows):
        src = pl.ds(pl.multiple_of(k * ALIGN, ALIGN), rows)
        dst = pl.ds(pl.multiple_of(cnt_ref[NSEQ + s] + k * ALIGN, ALIGN), rows)
        return pltpu.make_async_copy(gath_ref.at[s, src], stage.at[dst], g_sem.at[s, k])

    def each(s, op):
        many = 8
        full = cnt_ref[s] // (many * ALIGN)

        @pl.loop(0, full)
        def _(k):
            op(copy(s, k * many, many * ALIGN))

        @pl.loop(full * many, (cnt_ref[s] + ALIGN - 1) // ALIGN)
        def _(k):
            op(copy(s, k, ALIGN))

    for s in range(NSEQ):
        each(s, lambda cp: cp.start())
    last = NSEQ - 1
    end = cnt_ref[NSEQ + last] + (cnt_ref[last] + ALIGN - 1) // ALIGN * ALIGN

    blocks = cnt_ref[2 * NSEQ]

    @pl.loop(end // ALIGN, blocks * (S // ALIGN))
    def _(k):
        stage[pl.ds(pl.multiple_of(k * ALIGN, ALIGN), ALIGN), :] = jnp.zeros((ALIGN, E), F32)

    lanes = lax.broadcasted_iota(jnp.int32, (8, NTOK), 1)
    rows = jnp.where(lax.broadcasted_iota(jnp.int32, (8, NTOK), 0) == 2, 1e30, 0.0)
    loss = jnp.zeros((1, S), F32)
    for s in range(NSEQ):
        st = stats_ref[s]
        wide = jnp.concatenate([st, jnp.zeros((8, NTOK - S), F32)], axis=1)
        at = cnt_ref[NSEQ + s]
        rows = jnp.where((lanes >= at) & (lanes < at + cnt_ref[s]), pltpu.roll(wide, at, axis=1), rows)
        logz, tgt, w = st[1:2], st[4:5], st[5:6]
        loss = loss + jnp.where(w > 0.0, w * (logz - tgt + Z_WEIGHT * logz * logz), 0.0)
    rows_ref[...] = rows
    loss_ref[0, 0] = jnp.sum(loss / stats_ref[0, 6:7, :])
    for s in range(NSEQ):
        each(s, lambda cp: cp.wait())

    def put(b):
        at = pl.ds(pl.multiple_of(b * S, S), S)
        return pltpu.make_async_copy(hbuf.at[at], hc_ref.at[at], h_sem.at[b])

    @pl.loop(0, blocks)
    def _(b):
        for q in range(S // 64):
            at = pl.ds(pl.multiple_of(b * S + q * 64, 64), 64)
            hbuf[at, :] = stage[at, :].astype(BF16)
        put(b).start()

    @pl.loop(0, blocks)
    def _(b):
        put(b).wait()


def pack(cnt, stats, gath):
    vm = pl.BlockSpec(memory_space=pltpu.VMEM)
    sm = pl.BlockSpec(memory_space=pltpu.SMEM)
    hbm = pl.BlockSpec(memory_space=pl.ANY)
    return pl.pallas_call(
        _pack,
        out_shape=(jax.ShapeDtypeStruct((NTOK, E), BF16), jax.ShapeDtypeStruct((8, NTOK), F32), jax.ShapeDtypeStruct((1, 1), F32)),
        in_specs=[sm, vm, hbm], out_specs=(hbm, vm, sm),
        scratch_shapes=[pltpu.VMEM((NTOK, E), F32), pltpu.VMEM((NTOK, E), BF16), pltpu.SemaphoreType.DMA((NSEQ, S // ALIGN)),
                        pltpu.SemaphoreType.DMA((NTOK // S,))],
        compiler_params=pltpu.CompilerParams(vmem_limit_bytes=60 * 1024 * 1024),
        name="pack",
    )(cnt, stats, gath)


def _tail(x_ref, w_ref, g_ref, ln_ref, d0_ref, d1_ref, d2_ref, d3_ref, out_ref, dln_ref, xc, dc):
    i0 = lax.broadcasted_iota(jnp.int32, (S, S), 0)
    dest = _places(w_ref[...])
    dln = ln_ref[0]
    for q in range(1, 16):
        dln = dln + ln_ref[q]
    dln_ref[...] = dln
    pick = jnp.where(i0 == dest.astype(jnp.int32), 1.0, 0.0).astype(BF16)
    xc[...] = jnp.dot(pick, x_ref[...], preferred_element_type=F32)

    @pl.loop(0, S // LNR)
    def _(r):
        rows = pl.ds(pl.multiple_of(r * LNR, LNR), LNR)
        h, inv = _norm(xc[rows, :])
        a = ((d0_ref[rows, :] + d1_ref[rows, :]) + (d2_ref[rows, :] + d3_ref[rows, :])) * g_ref[...]
        d = inv * (a - jnp.mean(a, axis=-1, keepdims=True) - h * jnp.mean(a * h, axis=-1, keepdims=True))
        dc[rows, :] = d.astype(BF16)

    i1 = lax.broadcasted_iota(jnp.int32, (S, S), 1)
    back = jnp.where(_to_cols(jnp.broadcast_to(dest, (8, S)))[:, 0:1].astype(jnp.int32) == i1, 1.0, 0.0).astype(BF16)
    out_ref[...] = jnp.dot(back, dc[...], preferred_element_type=F32).astype(BF16)


def tail(x, w, g, ln, parts):
    vm = pl.BlockSpec(memory_space=pltpu.VMEM)
    return pl.pallas_call(
        _tail, out_shape=(jax.ShapeDtypeStruct((S, E), BF16), jax.ShapeDtypeStruct((1, E), F32)), in_specs=[vm] * 8, out_specs=(vm, vm),
        scratch_shapes=[pltpu.VMEM((S, E), F32), pltpu.VMEM((S, E), BF16)],
        compiler_params=pltpu.CompilerParams(vmem_limit_bytes=40 * 1024 * 1024), name="tail",
    )(x, w, g, ln, *parts)


def _dlogits(n, hc_ref, rows_ref, emb_ref, part_ref, dl_ref, all16, hc, ebuf, sbuf, h_sem, e_sem, w_sem, ss, rs, p_ss, p_rs):
    tp = lax.axis_index("tp")
    dp = lax.axis_index("dp")
    core = lax.rem(dp, 2)
    sib = _flip(dp, 1)
    nblk = VH // VB1
    steps = nblk // GROUP * TURN
    bar = pltpu.get_barrier_semaphore()
    others = [(z, k) for z in (0, 1) for k in range(8) if z or k]
    for z, k in others:
        pl.semaphore_signal(bar, inc=1, device_id=_dev(tp, dp, z, k), device_id_type=MESH)

    def row_of(i):
        q, k = i // TURN, lax.rem(i, TURN)
        extra = k // GROUP
        half = core + extra * (1 - 2 * core)
        return pl.multiple_of(half * VH + (q * GROUP + k - extra) * VB1, VB1)

    def emb_copy(i):
        slot = lax.rem(i, 2)
        return pltpu.make_async_copy(emb_ref.at[pl.ds(row_of(i), VB1)], ebuf.at[slot], e_sem.at[slot])

    def out_copy(i):
        slot = lax.rem(i, SLOTS)
        return pltpu.make_async_copy(sbuf.at[slot], dl_ref.at[pl.ds(row_of(i), VB1)], w_sem.at[slot])

    def send_copy(i):
        slot = lax.rem(i, SLOTS)
        rows = pl.ds(row_of(i), VB1)
        return pltpu.make_async_remote_copy(src_ref=sbuf.at[slot], dst_ref=dl_ref.at[rows], send_sem=ss.at[slot],
                                            recv_sem=rs.at[i // TURN * SENT + lax.rem(i, TURN)], device_id={"dp": sib}, device_id_type=MESH)

    h_copy = pltpu.make_async_copy(hc_ref.at[pl.ds(0, n)], hc, h_sem)
    h_copy.start()
    emb_copy(0).start()
    me = tp * 8 + dp
    all16[me] = part_ref[...]
    pl.semaphore_wait(bar, 15)
    part_cp = [_remote(part_ref, all16.at[me], p_ss.at[z * 8 + k], p_rs.at[z * 8 + k], _dev(tp, dp, z, k)) for z, k in others]
    for c in part_cp:
        c.start()
    h_copy.wait()
    shift, coef_b = rows_ref[2:3, :n], rows_ref[3:4, :n]
    sub = lax.broadcasted_iota(jnp.int32, (VB1, n), 0)

    @pl.loop(0, steps)
    def _(i):
        slot = lax.rem(i, SLOTS)
        emb_copy(i).wait()

        @pl.when(i + 1 < steps)
        def _():
            emb_copy(i + 1).start()

        @pl.when(i >= SLOTS)
        def _():
            out_copy(i - SLOTS).wait()

            @pl.when(lax.rem(i - SLOTS, TURN) < SENT)
            def _():
                send_copy(i - SLOTS).wait_send()

        yy = rows_ref[0:1, :n].astype(jnp.int32) - (tp * VT + row_of(i))
        l = lax.dot_general(ebuf[lax.rem(i, 2)], hc[...], NT, preferred_element_type=F32)
        p = jnp.exp2(l * LOG2E - shift)
        sbuf[slot] = jnp.where(sub == yy, p - coef_b, p)
        out_copy(i).start()

        @pl.when(lax.rem(i, TURN) < SENT)
        def _():
            send_copy(i).start()

    for i in range(steps - SLOTS, steps):
        out_copy(i).wait()
        if i % TURN < SENT:
            send_copy(i).wait_send()

    @pl.loop(0, nblk // GROUP * SENT)
    def _(i):
        send_copy(i // SENT * TURN + lax.rem(i, SENT)).wait_recv()
    for c in part_cp:
        c.wait()


def dlogits(n, cid, hc, rows, emb, part):
    dma = pltpu.SemaphoreType.DMA
    vm = pl.BlockSpec(memory_space=pltpu.VMEM)
    hbm = pl.BlockSpec(memory_space=pl.ANY)
    return pl.pallas_call(
        functools.partial(_dlogits, n),
        out_shape=(jax.ShapeDtypeStruct((VT, n), F32), jax.ShapeDtypeStruct((16, 1, E), F32)),
        in_specs=[hbm, vm, hbm, vm], out_specs=(hbm, vm),
        scratch_shapes=[pltpu.VMEM((n, E), BF16), pltpu.VMEM((2, VB1, E), BF16), pltpu.VMEM((SLOTS, VB1, n), F32),
                        dma, dma((2,)), dma((SLOTS,)), dma((SLOTS,)), dma((VH // VB1 // GROUP * SENT,)), dma((16,)), dma((16,))],
        compiler_params=pltpu.CompilerParams(collective_id=cid, has_side_effects=True, vmem_limit_bytes=60 * 1024 * 1024),
        cost_estimate=pl.CostEstimate(flops=2 * VH * n * E, bytes_accessed=VH * E * 2 + 2 * VH * n * 4, transcendentals=0),
        name=f"dlogits{n}",
    )(hc, rows, emb, part)


def _demb(dl_ref, hc_ref, out_ref):
    out_ref[...] = jnp.dot(dl_ref[...].astype(BF16), hc_ref[...], preferred_element_type=F32)


def demb(n, dl, hc):
    vb = 1024 if n < 2048 else 256
    return pl.pallas_call(
        _demb, grid=(VT // vb,),
        out_shape=jax.ShapeDtypeStruct((VT, E), F32),
        in_specs=[pl.BlockSpec((vb, n), lambda i: (i, 0)), pl.BlockSpec((n, E), lambda i: (0, 0), pipeline_mode=pl.Buffered(1))],
        out_specs=pl.BlockSpec((vb, E), lambda i: (i, 0)),
        compiler_params=pltpu.CompilerParams(dimension_semantics=("arbitrary",), vmem_limit_bytes=60 * 1024 * 1024),
        cost_estimate=pl.CostEstimate(flops=2 * VT * n * E, bytes_accessed=VT * E * 4 + VT * n * 4, transcendentals=0),
        name=f"demb{n}",
    )(dl, hc)


def solution(mesh):
    swap_core = [(i, i ^ 1) for i in range(16)]
    swap_both = [(i, i ^ 9) for i in range(16)]

    def local_step(hidden, targets, weights, embedding, ln_scale):
        x = hidden[0]
        g = ln_scale[None, :]
        gath, stats, mine, other, part, cnt, which = front(x, weights, targets, g, embedding)
        from_sib = lax.ppermute(other, ("tp", "dp"), swap_core)
        from_z = lax.ppermute(mine, "tp", [(0, 1), (1, 0)])
        from_both = lax.ppermute(other, ("tp", "dp"), swap_both)
        hc, rows, loss = pack(cnt, stats, gath)

        def back_of(i, n):
            def run(hc, rows, emb, part):
                dl, ln = dlogits(n, 1 + i, hc, rows, emb, part)
                return demb(n, dl, hc), ln
            return run

        d_emb, ln = lax.switch(which[0], [back_of(i, n) for i, n in enumerate(BUCKETS)], hc, rows, embedding, part)
        d_hidden, dln = tail(x, weights, g, ln, (mine, from_sib, from_z, from_both))
        return loss[0, 0], d_hidden[None], d_emb, dln[0]

    return jax.shard_map(local_step, mesh=mesh,
                         in_specs=(P("dp", None, None), P("dp", None), P("dp", None), P("tp", None), P(None)),
                         out_specs=(P(), P("dp", None, None), P("tp", None), P(None)), check_vma=False)
```

```python
import functools

import jax
import jax.numpy as jnp
from jax import lax
from jax.experimental import pallas as pl
from jax.experimental.pallas import tpu as pltpu
from jax.sharding import PartitionSpec as P

LN_EPS = 1e-6
Z_WEIGHT = 1e-4
LOG2E = 1.4426950408889634
LN2 = 0.6931471805599453
MESH = pl.DeviceIdType.MESH
F32 = jnp.float32
BF16 = jnp.bfloat16

S = 256
E = 2048
S2 = S + S
LANE = 128
LIMIT = 62914560
VT = 24576
VH = VT // 2
NSEQ = 8
NTOK = NSEQ * S
SIZES = ((768, 256, 256), (1024, 512, 512), (1280, 512, 512), (1536, 512, 256), (2048, 128, 32))
BUCKETS = [n for n, _, _ in SIZES]
ALIGN = 8

VBA = 2048
NBA = VH // VBA
LNR = 64

SLOTS = 5
GROUP, SENT, TURN = 12, 11, 13

NT = (((1,), (1,)), ((), ()))
NN = (((1,), (0,)), ((), ()))


def _flip(dp, k):
    out = dp
    for bit in (1, 2, 4):
        if k & bit:
            out = out + bit * (1 - 2 * lax.rem(dp // bit, 2))
    return out


def _dev(tp, dp, z, k):
    return {"tp": tp + z * (1 - 2 * tp), "dp": _flip(dp, k)}


def _remote(src, dst, ss, rs, dev):
    return pltpu.make_async_remote_copy(src_ref=src, dst_ref=dst, send_sem=ss, recv_sem=rs, device_id=dev, device_id_type=MESH)


def _to_cols(rows8):
    return jnp.transpose(jnp.concatenate([rows8, jnp.zeros((120, rows8.shape[1]), F32)], axis=0))


def _places(w):
    i0 = lax.broadcasted_iota(jnp.int32, (S, S), 0)
    i1 = lax.broadcasted_iota(jnp.int32, (S, S), 1)
    flags = jnp.broadcast_to(jnp.where(w > 0.0, 1.0, 0.0), (8, S)).astype(BF16)
    pos = jnp.dot(flags, jnp.where(i0 < i1, 1.0, 0.0).astype(BF16), preferred_element_type=F32)[0:1]
    return jnp.where(w > 0.0, pos, -1.0)


def _choose(index, *values):
    *first, out = values
    for i, v in enumerate(first):
        out = jnp.where(index == i, v, out)
    return out


def _norm(xf):
    cen = xf - jnp.mean(xf, axis=-1, keepdims=True)
    inv = lax.rsqrt(jnp.mean(cen * cen, axis=-1, keepdims=True) + LN_EPS)
    return cen * inv, inv


def _front(x_ref, w_ref, y_ref, g_ref, emb_ref, gath_ref, stats_ref, own_ref, sib_ref, dln_ref, cnt_ref, which_ref,
           hnf, xh, hn2, lg, ebuf, dlbuf, acc, m_s, s_s, t_s, bz, bb, by, wyc, wy_all, st4,
           e_sem, l_sem, row_ss, row_rs, wy_ss, wy_rs, st_ss, st_rs, sq_ss, sq_rs):
    tp = lax.axis_index("tp")
    dp = lax.axis_index("dp")
    core = lax.rem(dp, 2)
    sib = _flip(dp, 1)
    dpx, dpy, dpd = _flip(dp, 2), _flip(dp, 4), _flip(dp, 6)
    here = tp * 2 + core
    bar = pltpu.get_barrier_semaphore()
    for k in range(1, 8):
        pl.semaphore_signal(bar, inc=1, device_id=_dev(tp, dp, 0, k), device_id_type=MESH)
    for k in (0, 1):
        pl.semaphore_signal(bar, inc=1, device_id=_dev(tp, dp, 1, k), device_id_type=MESH)

    def emb_copy(j):
        row = pl.multiple_of(core * VH + j * VBA, VBA)
        slot = lax.rem(j, 2)
        return pltpu.make_async_copy(emb_ref.at[pl.ds(row, VBA)], ebuf.at[slot], e_sem.at[slot])

    emb_copy(0).start()
    i0 = lax.broadcasted_iota(jnp.int32, (S, S), 0)
    hit = i0 == _places(w_ref[...]).astype(jnp.int32)
    xc, xc_sib = acc.at[0:S], acc.at[S:S2]
    xc[...] = jnp.dot(jnp.where(hit, 1.0, 0.0).astype(BF16), x_ref[...], preferred_element_type=F32)
    wc = jnp.sum(jnp.where(hit, w_ref[...], 0.0), axis=1, keepdims=True)
    yc = jnp.sum(jnp.where(hit, y_ref[...].astype(F32), 0.0), axis=1, keepdims=True)
    ln = lax.broadcasted_iota(jnp.int32, (S, LANE), 1)
    wyc[...] = jnp.transpose(_choose(ln, wc, yc, 0.0))[0:8, :]
    wy_all[dp] = wyc[...]

    def layer_norm(src, half, keep):
        @pl.loop(0, S // LNR)
        def _(r):
            rows = pl.ds(pl.multiple_of(r * LNR, LNR), LNR)
            at = pl.ds(pl.multiple_of(half * S + r * LNR, LNR), LNR)
            h, _ = _norm(src[rows, :])
            xh[at, :] = h
            b = (h * g_ref[...]).astype(BF16)
            hn2[at, :] = b
            if keep:
                hnf[rows, :] = b.astype(F32)

    layer_norm(xc, core, True)
    pl.semaphore_wait(bar, 9)

    def rcopy(k, src, dst, dev):
        return _remote(src, dst, row_ss.at[k], row_rs.at[k], dev)

    Q = S // 4

    def quarter(k, part=0, parts=1):
        q = k + tp * (3 - 2 * k)
        return pl.ds(pl.multiple_of(q * Q + part * (Q // parts), 8), Q // parts)

    to_x, to_y, to_sib, to_z = _dev(tp, dp, 0, 2), _dev(tp, dp, 0, 4), _dev(tp, dp, 0, 1), _dev(tp, dp, 1, 0)
    x_cp = rcopy(0, xc, xc_sib, to_sib)

    def onward(k, q, rows, dev):
        return rcopy(k, gath_ref.at[q, rows], gath_ref.at[q, rows], dev)

    ex = [rcopy(1 + k, hnf.at[quarter(k)], gath_ref.at[dp, quarter(k)], to_x) for k in range(3)]
    ey = [rcopy(4 + k, hnf.at[quarter(k)], gath_ref.at[dp, quarter(k)], to_y) for k in range(3)]
    d0, d1 = onward(7, dpx, quarter(0), to_y), onward(8, dpy, quarter(1), to_x)
    d2, d3 = onward(9, dpx, quarter(2, 0, 2), to_y), onward(10, dpy, quarter(2, 1, 2), to_x)
    zx, zy, zd = (onward(11 + i, q, quarter(0), to_z) for i, q in enumerate((dpx, dpy, dpd)))
    fx, fy, fd = ([onward(14 + 4 * i + k, q, quarter(k), to_sib) for k in range(4)] for i, q in enumerate((dpx, dpy, dpd)))
    f_own = onward(26, dp, pl.ds(0, S), to_sib)
    wy_cp = [_remote(wyc, wy_all.at[dp], wy_ss.at[k], wy_rs.at[k], _dev(tp, dp, 0, k)) for k in range(1, 8)]
    x_cp.start()
    for c in wy_cp:
        c.start()

    for c in (ex[0], ey[1], ex[1], ey[0]):
        c.start()
    own_cp = pltpu.make_async_copy(hnf, gath_ref.at[dp], l_sem.at[0])
    own_cp.start()
    for c in wy_cp:
        c.wait()
    first = dp - core
    wrow = jnp.concatenate([wy_all[first, 0:1], wy_all[first + 1, 0:1]], axis=1)
    yrow = jnp.concatenate([wy_all[first, 1:2], wy_all[first + 1, 1:2]], axis=1)
    cols = _to_cols(jnp.broadcast_to(yrow, (8, S2)))
    by[...] = jnp.broadcast_to(cols[:, 0:1], (S2, LANE)).astype(jnp.int32)
    m_s[...] = jnp.full((S2, LANE), -1e30, F32)
    s_s[...] = jnp.zeros((S2, LANE), F32)
    t_s[...] = jnp.zeros((S2, LANE), F32)
    lane = lax.broadcasted_iota(jnp.int32, (S2, LANE), 1)
    base = tp * VT + core * VH
    x_cp.wait_recv()
    layer_norm(xc_sib, 1 - core, False)
    x_cp.wait_send()
    acc[...] = jnp.zeros((S2, E), F32)

    @pl.loop(0, NBA)
    def _(j):
        slot = lax.rem(j, 2)
        emb_copy(j).wait()

        @pl.when(j + 1 < NBA)
        def _():
            emb_copy(j + 1).start()

        @pl.when(j == 2)
        def _():
            ex[0].wait_recv()
            for c in (d0, zx):
                c.start()
            ey[1].wait_recv()
            for c in (d1, ex[2], ey[2], fx[0], fy[1]):
                c.start()

        @pl.when(j == 4)
        def _():
            ey[0].wait_recv()
            for c in (zy, fy[0]):
                c.start()
            ex[1].wait_recv()
            fx[1].start()

        l = lax.dot_general(hn2[...], ebuf[slot], NT, preferred_element_type=F32) * LOG2E
        lg[j] = l
        parts = [l[:, c * LANE:(c + 1) * LANE] for c in range(VBA // LANE)]
        mx = m_s[...]
        for p in parts:
            mx = jnp.maximum(mx, p)
        s = s_s[...] * jnp.exp2(m_s[...] - mx)
        t = t_s[...]
        yy = by[...] - (base + j * VBA)
        for c, p in enumerate(parts):
            s = s + jnp.exp2(p - mx)
            t = jnp.where(yy == lane + c * LANE, p, t)
        m_s[...] = mx
        s_s[...] = s
        t_s[...] = t

    emb_copy(0).start()
    mx = jnp.max(m_s[...], axis=1, keepdims=True)
    sm = jnp.sum(s_s[...] * jnp.exp2(m_s[...] - mx), axis=1, keepdims=True)
    tg = jnp.sum(t_s[...], axis=1, keepdims=True)
    packed = _choose(lane, mx, sm, tg, 0.0)
    st4[here] = jnp.transpose(packed)[0:8, :]
    st_cp = [_remote(st4.at[here], st4.at[here], st_ss.at[i], st_rs.at[i], _dev(tp, dp, z, k))
             for i, (z, k) in enumerate(((0, 1), (1, 0), (1, 1)))]
    for c in st_cp:
        c.start()
    w8 = jnp.concatenate([wy_all[q, 0:1] for q in range(NSEQ)], axis=0)
    total = jnp.sum(w8)
    start = jnp.int32(0)
    for q in range(NSEQ):
        cnt = jnp.sum(jnp.where(w8[q:q + 1] > 0.0, 1.0, 0.0)).astype(jnp.int32)
        cnt_ref[q] = cnt
        cnt_ref[NSEQ + q] = start
        start = start + (cnt + ALIGN - 1) // ALIGN * ALIGN
    which = sum((start > t).astype(jnp.int32) for t in BUCKETS[:-1])
    which_ref[0] = which
    cnt_ref[2 * NSEQ] = BUCKETS[0] // S + sum((which > i).astype(jnp.int32) * ((BUCKETS[i + 1] - BUCKETS[i]) // S) for i in range(len(BUCKETS) - 1))
    own_cp.wait()
    f_own.start()
    d0.wait_recv()
    for c in (zd, fd[0]):
        c.start()
    d1.wait_recv()
    fd[1].start()
    for c in st_cp:
        c.wait()
    ms = [st4[q, 0:1] for q in range(4)]
    mg = jnp.maximum(jnp.maximum(ms[0], ms[1]), jnp.maximum(ms[2], ms[3]))
    sg = jnp.zeros_like(mg)
    tgr = jnp.zeros_like(mg)
    for q in range(4):
        sg = sg + st4[q, 1:2] * jnp.exp2(ms[q] - mg)
        tgr = tgr + st4[q, 2:3]
    logz = (mg + jnp.log2(sg)) * LN2
    tgr = tgr * LN2
    coef_b = wrow * (jnp.full((1, S2), float(NTOK), F32) / total)
    coef_a = coef_b * (1.0 + 2.0 * Z_WEIGHT * logz)
    shift = jnp.where(coef_a > 0.0, mg + jnp.log2(sg) - jnp.log2(coef_a), 1e30)
    sub = lax.broadcasted_iota(jnp.int32, (8, S2), 0)
    rows8 = _choose(sub, yrow, logz, shift, coef_b, tgr, wrow, total)
    stats_ref[dp] = jnp.where(core == 0, rows8[:, :S], rows8[:, S:])
    sq_cp = [_remote(stats_ref.at[dp], stats_ref.at[dp], sq_ss.at[k], sq_rs.at[k], _dev(tp, dp, 0, k)) for k in range(1, 8)]
    for c in sq_cp:
        c.start()
    cols = _to_cols(rows8)
    bz[...] = jnp.broadcast_to(cols[:, 2:3], (S2, LANE))
    bb[...] = jnp.broadcast_to(cols[:, 3:4], (S2, LANE))

    @pl.loop(0, NBA)
    def _(j):
        slot = lax.rem(j, 2)
        emb_copy(j).wait()

        @pl.when(j + 1 < NBA)
        def _():
            emb_copy(j + 1).start()

        @pl.when(j == NBA // 3)
        def _():
            ex[2].wait_recv()
            for c in (d2, fx[2]):
                c.start()
            ey[2].wait_recv()
            for c in (d3, fy[2]):
                c.start()
            zx.wait_recv()
            fx[3].start()
            zy.wait_recv()
            fy[3].start()

        @pl.when(j == NBA - 1)
        def _():
            d2.wait_recv()
            d3.wait_recv()
            fd[2].start()

        yy = by[...] - (base + j * VBA)
        z, b = bz[...], bb[...]
        for c in range(VBA // LANE):
            p = jnp.exp2(lg[j, :, c * LANE:(c + 1) * LANE] - z)
            dlbuf[:, c * LANE:(c + 1) * LANE] = jnp.where(yy == lane + c * LANE, p - b, p).astype(BF16)
        acc[...] += lax.dot_general(dlbuf[...], ebuf[slot], NN, preferred_element_type=F32)

    own_out = pltpu.make_async_copy(acc.at[pl.ds(pl.multiple_of(core * S, S), S)], own_ref, l_sem.at[0])
    sib_out = pltpu.make_async_copy(acc.at[pl.ds(pl.multiple_of((1 - core) * S, S), S)], sib_ref, l_sem.at[1])
    own_out.start()
    sib_out.start()
    zd.wait_recv()
    fd[3].start()
    def add(q, dln):
        for r in range(4):
            at = pl.ds(pl.multiple_of(q * 32 + r * 8, 8), 8)
            dln = dln + acc[at, :] * xh[at, :]
        return dln

    dln_ref[...] = jnp.sum(lax.fori_loop(0, S2 // 32, add, jnp.zeros((8, E), F32)), axis=0, keepdims=True)
    for c in sq_cp:
        c.wait()
    own_out.wait()
    sib_out.wait()
    for c in ex + ey + [d0, d1, d2, d3, zx, zy, zd]:
        c.wait_send()
    for c in fx + fy + fd + [f_own]:
        c.wait()


def front(x, w, y, g, emb):
    vm = pl.BlockSpec(memory_space=pltpu.VMEM)
    hbm = pl.BlockSpec(memory_space=pl.ANY)
    dma = pltpu.SemaphoreType.DMA
    sm = pl.BlockSpec(memory_space=pltpu.SMEM)
    tile = pltpu.VMEM((S2, LANE), F32)
    seq = jax.ShapeDtypeStruct((S, E), F32)
    return pl.pallas_call(
        _front,
        out_shape=(jax.ShapeDtypeStruct((NSEQ, S, E), F32), jax.ShapeDtypeStruct((NSEQ, 8, S), F32), seq, seq,
                   jax.ShapeDtypeStruct((1, E), F32), jax.ShapeDtypeStruct((32,), jnp.int32), jax.ShapeDtypeStruct((1,), jnp.int32)),
        in_specs=[vm, vm, vm, vm, hbm], out_specs=(hbm, vm, hbm, hbm, vm, sm, sm),
        scratch_shapes=[
            pltpu.VMEM((S, E), F32), pltpu.VMEM((S2, E), F32), pltpu.VMEM((S2, E), BF16),
            pltpu.VMEM((NBA, S2, VBA), F32), pltpu.VMEM((2, VBA, E), BF16), pltpu.VMEM((S2, VBA), BF16),
            pltpu.VMEM((S2, E), F32), tile, tile, tile, tile, tile, pltpu.VMEM((S2, LANE), jnp.int32),
            pltpu.VMEM((8, S), F32), pltpu.VMEM((NSEQ, 8, S), F32), pltpu.VMEM((4, 8, S2), F32),
            dma((2,)), dma((2,)), dma((27,)), dma((27,)), dma((8,)), dma((8,)), dma((3,)), dma((3,)), dma((8,)), dma((8,)),
        ],
        compiler_params=pltpu.CompilerParams(collective_id=0, has_side_effects=True, vmem_limit_bytes=67043328),
        cost_estimate=pl.CostEstimate(flops=2 * 2 * S2 * VH * E, bytes_accessed=2 * VH * E * 2, transcendentals=0),
        name="front",
    )(x, w, y, g, emb)


def _pack(cnt_ref, stats_ref, gath_ref, hc_ref, rows_ref, loss_ref, stage, hbuf, g_sem, h_sem):
    def copy(s, k, rows):
        src = pl.ds(pl.multiple_of(k * ALIGN, ALIGN), rows)
        dst = pl.ds(pl.multiple_of(cnt_ref[NSEQ + s] + k * ALIGN, ALIGN), rows)
        return pltpu.make_async_copy(gath_ref.at[s, src], stage.at[dst], g_sem.at[s, k])

    def each(s, op):
        many = 8
        full = cnt_ref[s] // (many * ALIGN)

        @pl.loop(0, full)
        def _(k):
            op(copy(s, k * many, many * ALIGN))

        @pl.loop(full * many, (cnt_ref[s] + ALIGN - 1) // ALIGN)
        def _(k):
            op(copy(s, k, ALIGN))

    @pl.loop(0, NSEQ)
    def _(s):
        each(s, lambda cp: cp.start())

    last = NSEQ - 1
    end = cnt_ref[NSEQ + last] + (cnt_ref[last] + ALIGN - 1) // ALIGN * ALIGN

    blocks = cnt_ref[2 * NSEQ]

    @pl.loop(end // ALIGN, blocks * (S // ALIGN))
    def _(k):
        stage[pl.ds(pl.multiple_of(k * ALIGN, ALIGN), ALIGN), :] = jnp.zeros((ALIGN, E), F32)

    lanes = lax.broadcasted_iota(jnp.int32, (8, NTOK), 1)
    rows_ref[...] = jnp.where(lax.broadcasted_iota(jnp.int32, (8, NTOK), 0) == 2, 1e30, 0.0)

    def add(s, loss):
        st = stats_ref[s]
        wide = jnp.concatenate([st, jnp.zeros((8, NTOK - S), F32)], axis=1)
        at = cnt_ref[NSEQ + s]
        rows_ref[...] = jnp.where((lanes >= at) & (lanes < at + cnt_ref[s]), pltpu.roll(wide, at, axis=1), rows_ref[...])
        logz, tgt, w = st[1:2], st[4:5], st[5:6]
        return loss + jnp.where(w > 0.0, w * (logz - tgt + Z_WEIGHT * logz * logz), 0.0)

    loss = lax.fori_loop(0, NSEQ, add, jnp.zeros((1, S), F32))
    loss_ref[0, 0] = jnp.sum(loss / stats_ref[0, 6:7, :])


    def put(b):
        at = pl.ds(pl.multiple_of(b * S, S), S)
        return pltpu.make_async_copy(hbuf.at[at], hc_ref.at[at], h_sem.at[b])

    def convert(b):
        for q in range(S // 64):
            at = pl.ds(pl.multiple_of(b * S + q * 64, 64), 64)
            hbuf[at, :] = stage[at, :].astype(BF16)
        put(b).start()

    @pl.loop(0, NTOK // S)
    def _(b):
        @pl.loop(0, NSEQ)
        def _(s):
            @pl.when(cnt_ref[NSEQ + s] // S == b)
            def _():
                each(s, lambda cp: cp.wait())

        @pl.when(b < blocks)
        def _():
            convert(b)

    @pl.loop(0, blocks)
    def _(b):
        put(b).wait()


def pack(cnt, stats, gath):
    vm = pl.BlockSpec(memory_space=pltpu.VMEM)
    sm = pl.BlockSpec(memory_space=pltpu.SMEM)
    hbm = pl.BlockSpec(memory_space=pl.ANY)
    return pl.pallas_call(
        _pack,
        out_shape=(jax.ShapeDtypeStruct((NTOK, E), BF16), jax.ShapeDtypeStruct((8, NTOK), F32), jax.ShapeDtypeStruct((1, 1), F32)),
        in_specs=[sm, vm, hbm], out_specs=(hbm, vm, sm),
        scratch_shapes=[pltpu.VMEM((NTOK, E), F32), pltpu.VMEM((NTOK, E), BF16), pltpu.SemaphoreType.DMA((NSEQ, S // ALIGN)),
                        pltpu.SemaphoreType.DMA((NTOK // S,))],
        compiler_params=pltpu.CompilerParams(vmem_limit_bytes=LIMIT),
        name="pack",
    )(cnt, stats, gath)


def _tail(x_ref, w_ref, g_ref, ln_ref, d0_ref, d1_ref, d2_ref, d3_ref, out_ref, dln_ref, xc, dc):
    i0 = lax.broadcasted_iota(jnp.int32, (S, S), 0)
    dest = _places(w_ref[...])
    dln = ln_ref[0]
    for q in range(1, 16):
        dln = dln + ln_ref[q]
    dln_ref[...] = dln
    pick = jnp.where(i0 == dest.astype(jnp.int32), 1.0, 0.0).astype(BF16)
    xc[...] = jnp.dot(pick, x_ref[...], preferred_element_type=F32)

    @pl.loop(0, S // LNR)
    def _(r):
        rows = pl.ds(pl.multiple_of(r * LNR, LNR), LNR)
        h, inv = _norm(xc[rows, :])
        a = ((d0_ref[rows, :] + d1_ref[rows, :]) + (d2_ref[rows, :] + d3_ref[rows, :])) * g_ref[...]
        d = inv * (a - jnp.mean(a, axis=-1, keepdims=True) - h * jnp.mean(a * h, axis=-1, keepdims=True))
        dc[rows, :] = d.astype(BF16)

    i1 = lax.broadcasted_iota(jnp.int32, (S, S), 1)
    back = jnp.where(_to_cols(jnp.broadcast_to(dest, (8, S)))[:, 0:1].astype(jnp.int32) == i1, 1.0, 0.0).astype(BF16)
    out_ref[...] = jnp.dot(back, dc[...], preferred_element_type=F32).astype(BF16)


def tail(x, w, g, ln, parts):
    vm = pl.BlockSpec(memory_space=pltpu.VMEM)
    return pl.pallas_call(
        _tail, out_shape=(jax.ShapeDtypeStruct((S, E), BF16), jax.ShapeDtypeStruct((1, E), F32)), in_specs=[vm] * 8, out_specs=(vm, vm),
        scratch_shapes=[pltpu.VMEM((S, E), F32), pltpu.VMEM((S, E), BF16)],
        compiler_params=pltpu.CompilerParams(vmem_limit_bytes=LIMIT // 4), name="tail",
    )(x, w, g, ln, *parts)


def _dlogits(n, vb, hc_ref, rows_ref, emb_ref, part_ref, own_ref, sib_ref, all16, hc, ebuf, sbuf, bbuf, h_sem, e_sem, o_sem,
             x_sem, ss, rs, p_ss, p_rs):
    tp = lax.axis_index("tp")
    dp = lax.axis_index("dp")
    core = lax.rem(dp, 2)
    nblk = VH // vb
    steps = nblk // GROUP * TURN
    bar = pltpu.get_barrier_semaphore()
    others = [(z, k) for z in (0, 1) for k in range(8) if z or k]
    for z, k in others:
        pl.semaphore_signal(bar, inc=1, device_id=_dev(tp, dp, z, k), device_id_type=MESH)

    def place(i):
        q, k = i // TURN, lax.rem(i, TURN)
        extra = k // GROUP
        return extra, pl.multiple_of((q * GROUP + k - extra) * vb, vb)

    def row_of(i):
        extra, row = place(i)
        return pl.multiple_of((core + extra * (1 - 2 * core)) * VH + row, vb)

    def emb_copy(i):
        slot = lax.rem(i, 2)
        return pltpu.make_async_copy(emb_ref.at[pl.ds(row_of(i), vb)], ebuf.at[slot], e_sem.at[slot])

    def own_copy(i):
        slot = lax.rem(i, 2)
        return pltpu.make_async_copy(bbuf.at[slot], own_ref.at[pl.ds(place(i)[1], vb)], o_sem.at[slot])

    def extra_copy(i):
        slot = lax.rem(i, SLOTS)
        return pltpu.make_async_copy(sbuf.at[slot], sib_ref.at[pl.ds(place(i)[1], vb)], x_sem.at[slot])

    def send_copy(i):
        slot = lax.rem(i, SLOTS)
        return _remote(sbuf.at[slot], sib_ref.at[pl.ds(place(i)[1], vb)], ss.at[slot],
                       rs.at[i // TURN * SENT + lax.rem(i, TURN)], _dev(tp, dp, 0, 1))

    def free(i):
        @pl.when(lax.rem(i, TURN) < SENT)
        def _():
            send_copy(i).wait_send()

        @pl.when(lax.rem(i, TURN) == GROUP)
        def _():
            extra_copy(i).wait()

    h_copy = pltpu.make_async_copy(hc_ref.at[pl.ds(0, n)], hc, h_sem)
    h_copy.start()
    emb_copy(0).start()
    me = tp * 8 + dp
    all16[me] = part_ref[...]
    pl.semaphore_wait(bar, 15)
    part_cp = [_remote(part_ref, all16.at[me], p_ss.at[z * 8 + k], p_rs.at[z * 8 + k], _dev(tp, dp, z, k)) for z, k in others]
    for c in part_cp:
        c.start()
    h_copy.wait()
    shift, coef_b = rows_ref[2:3, :n], rows_ref[3:4, :n]
    sub = lax.broadcasted_iota(jnp.int32, (vb, n), 0)

    @pl.loop(0, steps)
    def _(i):
        emb_copy(i).wait()

        @pl.when(i + 1 < steps)
        def _():
            emb_copy(i + 1).start()

        @pl.when((i > 1) & (lax.rem(i - 2, TURN) < GROUP))
        def _():
            own_copy(i - 2).wait()

        @pl.when(i >= SLOTS)
        def _():
            free(i - SLOTS)

        yy = rows_ref[0:1, :n].astype(jnp.int32) - (tp * VT + row_of(i))
        l = lax.dot_general(ebuf[lax.rem(i, 2)], hc[...], NT, preferred_element_type=F32)
        p = jnp.exp2(l * LOG2E - shift)
        p = jnp.where(sub == yy, p - coef_b, p)
        sbuf[lax.rem(i, SLOTS)] = p
        bbuf[lax.rem(i, 2)] = p.astype(BF16)

        @pl.when(lax.rem(i, TURN) < SENT)
        def _():
            send_copy(i).start()

        @pl.when(lax.rem(i, TURN) < GROUP)
        def _():
            own_copy(i).start()

        @pl.when(lax.rem(i, TURN) == GROUP)
        def _():
            extra_copy(i).start()

    own_copy(steps - 2).wait()
    for i in range(SLOTS):
        free(steps - SLOTS + i)

    @pl.loop(0, nblk // GROUP * SENT)
    def _(i):
        send_copy(i // SENT * TURN + lax.rem(i, SENT)).wait_recv()
    for c in part_cp:
        c.wait()


def dlogits(n, vb, cid, hc, rows, emb, part):
    dma = pltpu.SemaphoreType.DMA
    vm = pl.BlockSpec(memory_space=pltpu.VMEM)
    hbm = pl.BlockSpec(memory_space=pl.ANY)
    return pl.pallas_call(
        functools.partial(_dlogits, n, vb),
        out_shape=(jax.ShapeDtypeStruct((VH, n), BF16), jax.ShapeDtypeStruct((VH, n), F32), jax.ShapeDtypeStruct((16, 1, E), F32)),
        in_specs=[hbm, vm, hbm, vm], out_specs=(hbm, hbm, vm),
        scratch_shapes=[pltpu.VMEM((n, E), BF16), pltpu.VMEM((2, vb, E), BF16), pltpu.VMEM((SLOTS, vb, n), F32),
                        pltpu.VMEM((2, vb, n), BF16), dma, dma((2,)), dma((2,)), dma((SLOTS,)), dma((SLOTS,)),
                        dma((VH // vb // GROUP * SENT,)), dma((16,)), dma((16,))],
        compiler_params=pltpu.CompilerParams(collective_id=cid, has_side_effects=True, vmem_limit_bytes=LIMIT),
        cost_estimate=pl.CostEstimate(flops=2 * VH * n * E, bytes_accessed=VH * E * 2 + 2 * VH * n * 4, transcendentals=0),
        name=f"dlogits{n}",
    )(hc, rows, emb, part)


def _demb(own_ref, sib_ref, hc_ref, out_ref):
    core = lax.rem(lax.axis_index("dp"), 2)
    out_ref[core] = jnp.dot(own_ref[...], hc_ref[...], preferred_element_type=F32)
    out_ref[1 - core] = jnp.dot(sib_ref[...].astype(BF16), hc_ref[...], preferred_element_type=F32)


def demb(n, vb, own, sib, hc):
    rows = pl.BlockSpec((vb, n), lambda i: (i, 0))
    return pl.pallas_call(
        _demb, grid=(VH // vb,),
        out_shape=jax.ShapeDtypeStruct((2, VH, E), F32),
        in_specs=[rows, rows, pl.BlockSpec((n, E), lambda i: (0, 0), pipeline_mode=pl.Buffered(1))],
        out_specs=pl.BlockSpec((2, vb, E), lambda i: (0, i, 0)),
        compiler_params=pltpu.CompilerParams(dimension_semantics=("arbitrary",), vmem_limit_bytes=LIMIT),
        cost_estimate=pl.CostEstimate(flops=2 * VT * n * E, bytes_accessed=VT * E * 4 + VT * n * 3, transcendentals=0),
        name=f"demb{n}",
    )(own, sib, hc).reshape(VT, E)


def solution(mesh):
    swap_core = [(i, i ^ 1) for i in range(16)]
    swap_both = [(i, i ^ 9) for i in range(16)]

    def local_step(hidden, targets, weights, embedding, ln_scale):
        x = hidden[0]
        g = ln_scale[None, :]
        gath, stats, mine, other, part, cnt, which = front(x, weights, targets, g, embedding)
        from_sib = lax.ppermute(other, ("tp", "dp"), swap_core)
        from_z = lax.ppermute(mine, "tp", [(0, 1), (1, 0)])
        from_both = lax.ppermute(other, ("tp", "dp"), swap_both)
        hc, rows, loss = pack(cnt, stats, gath)

        def back_of(i, n, rows1, rows2):
            def run(hc, rows, emb, part):
                own, sib, ln = dlogits(n, rows1, 1 + i, hc, rows, emb, part)
                return demb(n, rows2, own, sib, hc), ln
            return run

        d_emb, ln = lax.switch(which[0], [back_of(i, *size) for i, size in enumerate(SIZES)], hc, rows, embedding, part)
        d_hidden, dln = tail(x, weights, g, ln, (mine, from_sib, from_z, from_both))
        return loss[0, 0], d_hidden[None], d_emb, dln[0]

    return jax.shard_map(local_step, mesh=mesh,
                         in_specs=(P("dp", None, None), P("dp", None), P("dp", None), P("tp", None), P(None)),
                         out_specs=(P(), P("dp", None, None), P("tp", None), P(None)), check_vma=False)
```

```python
import functools

import jax
import jax.numpy as jnp
from jax import lax
from jax.experimental import pallas as pl
from jax.experimental.pallas import tpu as pltpu
from jax.sharding import PartitionSpec as P

LN_EPS = 1e-6
Z_WEIGHT = 1e-4
LOG2E = 1.4426950408889634
LN2 = 0.6931471805599453
MESH = pl.DeviceIdType.MESH
F32 = jnp.float32
BF16 = jnp.bfloat16

S = 256
E = 2048
S2 = S + S
LANE = 128
LIMIT = 62914560
OTHERS = (1, 16)
VT = 24576
VH = VT // 2
NSEQ = 8
NTOK = NSEQ * S
SIZES = ((768, 512, 256), (1024, 512, 512), (1280, 512, 512), (1536, 256, 256), (2048, 128, 32))
BUCKETS = [n for n, _, _ in SIZES]
ALIGN = 8

VBA = 2048
NBA = VH // VBA
LNR = 64

SLOTS = 5
GROUP, SENT, TURN = 12, 11, 13

NT = (((1,), (1,)), ((), ()))
NN = (((1,), (0,)), ((), ()))


def _flip(dp, k):
    out = dp
    for bit in (1, 2, 4):
        if k & bit:
            out = out + bit * (1 - 2 * lax.rem(dp // bit, 2))
    return out


def _dev(tp, dp, z, k):
    return {"tp": tp + z * (1 - 2 * tp), "dp": _flip(dp, k)}


def _remote(src, dst, ss, rs, dev):
    return pltpu.make_async_remote_copy(src_ref=src, dst_ref=dst, send_sem=ss, recv_sem=rs, device_id=dev, device_id_type=MESH)


def _to_cols(rows8):
    return jnp.transpose(jnp.concatenate([rows8, jnp.zeros((120, rows8.shape[1]), F32)], axis=0))


def _places(w):
    i0 = lax.broadcasted_iota(jnp.int32, (S, S), 0)
    i1 = lax.broadcasted_iota(jnp.int32, (S, S), 1)
    flags = jnp.broadcast_to(jnp.where(w > 0.0, 1.0, 0.0), (8, S)).astype(BF16)
    pos = jnp.dot(flags, jnp.where(i0 < i1, 1.0, 0.0).astype(BF16), preferred_element_type=F32)[0:1]
    return jnp.where(w > 0.0, pos, -1.0)


def _choose(index, *values):
    *first, out = values
    for i, v in enumerate(first):
        out = jnp.where(index == i, v, out)
    return out


def _norm(xf):
    cen = xf - jnp.mean(xf, axis=-1, keepdims=True)
    inv = lax.rsqrt(jnp.mean(cen * cen, axis=-1, keepdims=True) + LN_EPS)
    return cen * inv, inv


def _front(x_ref, w_ref, y_ref, g_ref, emb_ref, gath_ref, stats_ref, own_ref, sib_ref, dln_ref, cnt_ref, which_ref,
           hnf, xh, hn2, lg, ebuf, dlbuf, acc, m_s, s_s, t_s, bz, bb, by, wyc, wy_all, st4,
           e_sem, l_sem, row_ss, row_rs, wy_ss, wy_rs, st_ss, st_rs, sq_ss, sq_rs):
    tp = lax.axis_index("tp")
    dp = lax.axis_index("dp")
    core = lax.rem(dp, 2)
    sib = _flip(dp, 1)
    dpx, dpy, dpd = _flip(dp, 2), _flip(dp, 4), _flip(dp, 6)
    here = tp * 2 + core
    bar = pltpu.get_barrier_semaphore()
    for k in range(1, 8):
        pl.semaphore_signal(bar, inc=1, device_id=_dev(tp, dp, 0, k), device_id_type=MESH)
    for k in (0, 1):
        pl.semaphore_signal(bar, inc=1, device_id=_dev(tp, dp, 1, k), device_id_type=MESH)

    def emb_copy(j):
        row = pl.multiple_of(core * VH + j * VBA, VBA)
        slot = lax.rem(j, 2)
        return pltpu.make_async_copy(emb_ref.at[pl.ds(row, VBA)], ebuf.at[slot], e_sem.at[slot])

    emb_copy(0).start()
    i0 = lax.broadcasted_iota(jnp.int32, (S, S), 0)
    hit = i0 == _places(w_ref[...]).astype(jnp.int32)
    xc, xc_sib = acc.at[0:S], acc.at[S:S2]
    xc[...] = jnp.dot(jnp.where(hit, 1.0, 0.0).astype(BF16), x_ref[...], preferred_element_type=F32)
    wc = jnp.sum(jnp.where(hit, w_ref[...], 0.0), axis=1, keepdims=True)
    yc = jnp.sum(jnp.where(hit, y_ref[...].astype(F32), 0.0), axis=1, keepdims=True)
    ln = lax.broadcasted_iota(jnp.int32, (S, LANE), 1)
    wyc[...] = jnp.transpose(_choose(ln, wc, yc, 0.0))[0:8, :]
    wy_all[dp] = wyc[...]

    def layer_norm(src, half, keep):
        @pl.loop(0, S // LNR)
        def _(r):
            rows = pl.ds(pl.multiple_of(r * LNR, LNR), LNR)
            at = pl.ds(pl.multiple_of(half * S + r * LNR, LNR), LNR)
            h, _ = _norm(src[rows, :])
            xh[at, :] = h
            b = (h * g_ref[...]).astype(BF16)
            hn2[at, :] = b
            if keep:
                hnf[rows, :] = b.astype(F32)

    layer_norm(xc, core, True)
    pl.semaphore_wait(bar, 9)

    def rcopy(k, src, dst, dev):
        return _remote(src, dst, row_ss.at[k], row_rs.at[k], dev)

    Q = S // 4

    def quarter(k, part=0, parts=1):
        q = k + tp * (3 - 2 * k)
        return pl.ds(pl.multiple_of(q * Q + part * (Q // parts), 8), Q // parts)

    to_x, to_y, to_sib, to_z = _dev(tp, dp, 0, 2), _dev(tp, dp, 0, 4), _dev(tp, dp, 0, 1), _dev(tp, dp, 1, 0)
    x_cp = rcopy(0, xc, xc_sib, to_sib)

    def onward(k, q, rows, dev):
        return rcopy(k, gath_ref.at[q, rows], gath_ref.at[q, rows], dev)

    ex = [rcopy(1 + k, hnf.at[quarter(k)], gath_ref.at[dp, quarter(k)], to_x) for k in range(3)]
    ey = [rcopy(4 + k, hnf.at[quarter(k)], gath_ref.at[dp, quarter(k)], to_y) for k in range(3)]
    d0, d1 = onward(7, dpx, quarter(0), to_y), onward(8, dpy, quarter(1), to_x)
    d2, d3 = onward(9, dpx, quarter(2, 0, 2), to_y), onward(10, dpy, quarter(2, 1, 2), to_x)
    zx, zy, zd = (onward(11 + i, q, quarter(0), to_z) for i, q in enumerate((dpx, dpy, dpd)))
    fx, fy, fd = ([onward(14 + 4 * i + k, q, quarter(k), to_sib) for k in range(4)] for i, q in enumerate((dpx, dpy, dpd)))
    f_own = onward(26, dp, pl.ds(0, S), to_sib)
    wy_cp = [_remote(wyc, wy_all.at[dp], wy_ss.at[k], wy_rs.at[k], _dev(tp, dp, 0, k)) for k in range(1, 8)]
    x_cp.start()
    for c in wy_cp:
        c.start()

    for c in (ex[0], ey[1], ex[1], ey[0]):
        c.start()
    own_cp = pltpu.make_async_copy(hnf, gath_ref.at[dp], l_sem.at[0])
    own_cp.start()
    for c in wy_cp:
        c.wait()
    first = dp - core
    wrow = jnp.concatenate([wy_all[first, 0:1], wy_all[first + 1, 0:1]], axis=1)
    yrow = jnp.concatenate([wy_all[first, 1:2], wy_all[first + 1, 1:2]], axis=1)
    cols = _to_cols(jnp.broadcast_to(yrow, (8, S2)))
    by[...] = jnp.broadcast_to(cols[:, 0:1], (S2, LANE)).astype(jnp.int32)
    m_s[...] = jnp.full((S2, LANE), -1e30, F32)
    s_s[...] = jnp.zeros((S2, LANE), F32)
    t_s[...] = jnp.zeros((S2, LANE), F32)
    lane = lax.broadcasted_iota(jnp.int32, (S2, LANE), 1)
    base = tp * VT + core * VH
    x_cp.wait_recv()
    layer_norm(xc_sib, 1 - core, False)
    x_cp.wait_send()
    acc[...] = jnp.zeros((S2, E), F32)

    @pl.loop(0, NBA)
    def _(j):
        slot = lax.rem(j, 2)
        emb_copy(j).wait()

        @pl.when(j + 1 < NBA)
        def _():
            emb_copy(j + 1).start()

        @pl.when(j == 2)
        def _():
            ex[0].wait_recv()
            for c in (d0, zx):
                c.start()
            ey[1].wait_recv()
            for c in (d1, ex[2], ey[2], fx[0], fy[1]):
                c.start()

        @pl.when(j == 4)
        def _():
            ey[0].wait_recv()
            for c in (zy, fy[0]):
                c.start()
            ex[1].wait_recv()
            fx[1].start()

        l = lax.dot_general(hn2[...], ebuf[slot], NT, preferred_element_type=F32) * LOG2E
        lg[j] = l
        parts = [l[:, c * LANE:(c + 1) * LANE] for c in range(VBA // LANE)]
        mx = m_s[...]
        for p in parts:
            mx = jnp.maximum(mx, p)
        s = s_s[...] * jnp.exp2(m_s[...] - mx)
        t = t_s[...]
        yy = by[...] - (base + j * VBA)
        for c, p in enumerate(parts):
            s = s + jnp.exp2(p - mx)
            t = jnp.where(yy == lane + c * LANE, p, t)
        m_s[...] = mx
        s_s[...] = s
        t_s[...] = t

    emb_copy(0).start()
    mx = jnp.max(m_s[...], axis=1, keepdims=True)
    sm = jnp.sum(s_s[...] * jnp.exp2(m_s[...] - mx), axis=1, keepdims=True)
    tg = jnp.sum(t_s[...], axis=1, keepdims=True)
    packed = _choose(lane, mx, sm, tg, 0.0)
    st4[here] = jnp.transpose(packed)[0:8, :]
    st_cp = [_remote(st4.at[here], st4.at[here], st_ss.at[i], st_rs.at[i], _dev(tp, dp, z, k))
             for i, (z, k) in enumerate(((0, 1), (1, 0), (1, 1)))]
    for c in st_cp:
        c.start()
    w8 = jnp.concatenate([wy_all[q, 0:1] for q in range(NSEQ)], axis=0)
    total = jnp.sum(w8)
    start = jnp.int32(0)
    for q in range(NSEQ):
        cnt = jnp.sum(jnp.where(w8[q:q + 1] > 0.0, 1.0, 0.0)).astype(jnp.int32)
        cnt_ref[q] = cnt
        cnt_ref[NSEQ + q] = start
        start = start + (cnt + ALIGN - 1) // ALIGN * ALIGN
    which = sum((start > t).astype(jnp.int32) for t in BUCKETS[:-1])
    which_ref[0] = which
    cnt_ref[2 * NSEQ] = BUCKETS[0] // S + sum((which > i).astype(jnp.int32) * ((BUCKETS[i + 1] - BUCKETS[i]) // S) for i in range(len(BUCKETS) - 1))
    own_cp.wait()
    f_own.start()
    d0.wait_recv()
    for c in (zd, fd[0]):
        c.start()
    d1.wait_recv()
    fd[1].start()
    for c in st_cp:
        c.wait()
    ms = [st4[q, 0:1] for q in range(4)]
    mg = jnp.maximum(jnp.maximum(ms[0], ms[1]), jnp.maximum(ms[2], ms[3]))
    sg = jnp.zeros_like(mg)
    tgr = jnp.zeros_like(mg)
    for q in range(4):
        sg = sg + st4[q, 1:2] * jnp.exp2(ms[q] - mg)
        tgr = tgr + st4[q, 2:3]
    logz = (mg + jnp.log2(sg)) * LN2
    tgr = tgr * LN2
    coef_b = wrow * (jnp.full((1, S2), float(NTOK), F32) / total)
    coef_a = coef_b * (1.0 + 2.0 * Z_WEIGHT * logz)
    shift = jnp.where(coef_a > 0.0, mg + jnp.log2(sg) - jnp.log2(coef_a), 1e30)
    sub = lax.broadcasted_iota(jnp.int32, (8, S2), 0)
    rows8 = _choose(sub, yrow, logz, shift, coef_b, tgr, wrow, total)
    stats_ref[dp] = jnp.where(core == 0, rows8[:, :S], rows8[:, S:])
    sq_cp = [_remote(stats_ref.at[dp], stats_ref.at[dp], sq_ss.at[k], sq_rs.at[k], _dev(tp, dp, 0, k)) for k in range(1, 8)]
    for c in sq_cp:
        c.start()
    cols = _to_cols(rows8)
    bz[...] = jnp.broadcast_to(cols[:, 2:3], (S2, LANE))
    bb[...] = jnp.broadcast_to(cols[:, 3:4], (S2, LANE))

    @pl.loop(0, NBA)
    def _(j):
        slot = lax.rem(j, 2)
        emb_copy(j).wait()

        @pl.when(j + 1 < NBA)
        def _():
            emb_copy(j + 1).start()

        @pl.when(j == NBA // 3)
        def _():
            ex[2].wait_recv()
            for c in (d2, fx[2]):
                c.start()
            ey[2].wait_recv()
            for c in (d3, fy[2]):
                c.start()
            zx.wait_recv()
            fx[3].start()
            zy.wait_recv()
            fy[3].start()

        @pl.when(j == NBA - 1)
        def _():
            d2.wait_recv()
            d3.wait_recv()
            fd[2].start()

        yy = by[...] - (base + j * VBA)
        z, b = bz[...], bb[...]
        for c in range(VBA // LANE):
            p = jnp.exp2(lg[j, :, c * LANE:(c + 1) * LANE] - z)
            dlbuf[:, c * LANE:(c + 1) * LANE] = jnp.where(yy == lane + c * LANE, p - b, p).astype(BF16)
        acc[...] += lax.dot_general(dlbuf[...], ebuf[slot], NN, preferred_element_type=F32)

    own_out = pltpu.make_async_copy(acc.at[pl.ds(pl.multiple_of(core * S, S), S)], own_ref, l_sem.at[0])
    sib_out = pltpu.make_async_copy(acc.at[pl.ds(pl.multiple_of((1 - core) * S, S), S)], sib_ref, l_sem.at[1])
    own_out.start()
    sib_out.start()
    zd.wait_recv()
    fd[3].start()
    def add(q, dln):
        for r in range(4):
            at = pl.ds(pl.multiple_of(q * 32 + r * 8, 8), 8)
            dln = dln + acc[at, :] * xh[at, :]
        return dln

    dln_ref[...] = jnp.sum(lax.fori_loop(0, S2 // 32, add, jnp.zeros((8, E), F32)), axis=0, keepdims=True)
    for c in sq_cp:
        c.wait()
    own_out.wait()
    sib_out.wait()
    for c in ex + ey + [d0, d1, d2, d3, zx, zy, zd]:
        c.wait_send()
    for c in fx + fy + fd + [f_own]:
        c.wait()


def front(x, w, y, g, emb):
    vm = pl.BlockSpec(memory_space=pltpu.VMEM)
    hbm = pl.BlockSpec(memory_space=pl.ANY)
    dma = pltpu.SemaphoreType.DMA
    sm = pl.BlockSpec(memory_space=pltpu.SMEM)
    tile = pltpu.VMEM((S2, LANE), F32)
    seq = jax.ShapeDtypeStruct((S, E), F32)
    return pl.pallas_call(
        _front,
        out_shape=(jax.ShapeDtypeStruct((NSEQ, S, E), F32), jax.ShapeDtypeStruct((NSEQ, 8, S), F32), seq, seq,
                   jax.ShapeDtypeStruct((1, E), F32), jax.ShapeDtypeStruct((32,), jnp.int32), jax.ShapeDtypeStruct((1,), jnp.int32)),
        in_specs=[vm, vm, vm, vm, hbm], out_specs=(hbm, vm, hbm, hbm, vm, sm, sm),
        scratch_shapes=[
            pltpu.VMEM((S, E), F32), pltpu.VMEM((S2, E), F32), pltpu.VMEM((S2, E), BF16),
            pltpu.VMEM((NBA, S2, VBA), F32), pltpu.VMEM((2, VBA, E), BF16), pltpu.VMEM((S2, VBA), BF16),
            pltpu.VMEM((S2, E), F32), tile, tile, tile, tile, tile, pltpu.VMEM((S2, LANE), jnp.int32),
            pltpu.VMEM((8, S), F32), pltpu.VMEM((NSEQ, 8, S), F32), pltpu.VMEM((4, 8, S2), F32),
            dma((2,)), dma((2,)), dma((27,)), dma((27,)), dma((8,)), dma((8,)), dma((3,)), dma((3,)), dma((8,)), dma((8,)),
        ],
        compiler_params=pltpu.CompilerParams(collective_id=0, has_side_effects=True, vmem_limit_bytes=67043328),
        cost_estimate=pl.CostEstimate(flops=2 * 2 * S2 * VH * E, bytes_accessed=2 * VH * E * 2, transcendentals=0),
        name="front",
    )(x, w, y, g, emb)


def _pack(cnt_ref, stats_ref, gath_ref, hc_ref, rows_ref, loss_ref, stage, hbuf, g_sem, h_sem):
    def copy(s, k, rows):
        src = pl.ds(pl.multiple_of(k * ALIGN, ALIGN), rows)
        dst = pl.ds(pl.multiple_of(cnt_ref[NSEQ + s] + k * ALIGN, ALIGN), rows)
        return pltpu.make_async_copy(gath_ref.at[s, src], stage.at[dst], g_sem.at[s, k])

    def each(s, op):
        many = 8
        full = cnt_ref[s] // (many * ALIGN)

        @pl.loop(0, full)
        def _(k):
            op(copy(s, k * many, many * ALIGN))

        @pl.loop(full * many, (cnt_ref[s] + ALIGN - 1) // ALIGN)
        def _(k):
            op(copy(s, k, ALIGN))

    @pl.loop(0, NSEQ)
    def _(s):
        each(s, lambda cp: cp.start())

    last = NSEQ - 1
    end = cnt_ref[NSEQ + last] + (cnt_ref[last] + ALIGN - 1) // ALIGN * ALIGN

    blocks = cnt_ref[2 * NSEQ]

    @pl.loop(end // ALIGN, blocks * (S // ALIGN))
    def _(k):
        stage[pl.ds(pl.multiple_of(k * ALIGN, ALIGN), ALIGN), :] = jnp.zeros((ALIGN, E), F32)

    lanes = lax.broadcasted_iota(jnp.int32, (8, NTOK), 1)
    rows_ref[...] = jnp.where(lax.broadcasted_iota(jnp.int32, (8, NTOK), 0) == 2, 1e30, 0.0)

    def add(s, loss):
        st = stats_ref[s]
        wide = jnp.concatenate([st, jnp.zeros((8, NTOK - S), F32)], axis=1)
        at = cnt_ref[NSEQ + s]
        rows_ref[...] = jnp.where((lanes >= at) & (lanes < at + cnt_ref[s]), pltpu.roll(wide, at, axis=1), rows_ref[...])
        logz, tgt, w = st[1:2], st[4:5], st[5:6]
        return loss + jnp.where(w > 0.0, w * (logz - tgt + Z_WEIGHT * logz * logz), 0.0)

    loss = lax.fori_loop(0, NSEQ, add, jnp.zeros((1, S), F32))
    loss_ref[0, 0] = jnp.sum(loss / stats_ref[0, 6:7, :])


    def put(b):
        at = pl.ds(pl.multiple_of(b * S, S), S)
        return pltpu.make_async_copy(hbuf.at[at], hc_ref.at[at], h_sem.at[b])

    def convert(b):
        for q in range(S // 64):
            at = pl.ds(pl.multiple_of(b * S + q * 64, 64), 64)
            hbuf[at, :] = stage[at, :].astype(BF16)
        put(b).start()

    @pl.loop(0, NTOK // S)
    def _(b):
        @pl.loop(0, NSEQ)
        def _(s):
            @pl.when(cnt_ref[NSEQ + s] // S == b)
            def _():
                each(s, lambda cp: cp.wait())

        @pl.when(b < blocks)
        def _():
            convert(b)

    @pl.loop(0, blocks)
    def _(b):
        put(b).wait()


def pack(cnt, stats, gath):
    vm = pl.BlockSpec(memory_space=pltpu.VMEM)
    sm = pl.BlockSpec(memory_space=pltpu.SMEM)
    hbm = pl.BlockSpec(memory_space=pl.ANY)
    return pl.pallas_call(
        _pack,
        out_shape=(jax.ShapeDtypeStruct((NTOK, E), BF16), jax.ShapeDtypeStruct((8, NTOK), F32), jax.ShapeDtypeStruct((1, 1), F32)),
        in_specs=[sm, vm, hbm], out_specs=(hbm, vm, sm),
        scratch_shapes=[pltpu.VMEM((NTOK, E), F32), pltpu.VMEM((NTOK, E), BF16), pltpu.SemaphoreType.DMA((NSEQ, S // ALIGN)),
                        pltpu.SemaphoreType.DMA((NTOK // S,))],
        compiler_params=pltpu.CompilerParams(vmem_limit_bytes=LIMIT),
        name="pack",
    )(cnt, stats, gath)


def _tail(x_ref, w_ref, g_ref, ln_ref, d0_ref, d1_ref, d2_ref, d3_ref, out_ref, dln_ref, xc, dc):
    i0 = lax.broadcasted_iota(jnp.int32, (S, S), 0)
    dest = _places(w_ref[...])
    dln = ln_ref[0]
    for q in range(1, 16):
        dln = dln + ln_ref[q]
    dln_ref[...] = dln
    pick = jnp.where(i0 == dest.astype(jnp.int32), 1.0, 0.0).astype(BF16)
    xc[...] = jnp.dot(pick, x_ref[...], preferred_element_type=F32)

    @pl.loop(0, S // LNR)
    def _(r):
        rows = pl.ds(pl.multiple_of(r * LNR, LNR), LNR)
        h, inv = _norm(xc[rows, :])
        a = ((d0_ref[rows, :] + d1_ref[rows, :]) + (d2_ref[rows, :] + d3_ref[rows, :])) * g_ref[...]
        d = inv * (a - jnp.mean(a, axis=-1, keepdims=True) - h * jnp.mean(a * h, axis=-1, keepdims=True))
        dc[rows, :] = d.astype(BF16)

    i1 = lax.broadcasted_iota(jnp.int32, (S, S), 1)
    back = jnp.where(_to_cols(jnp.broadcast_to(dest, (8, S)))[:, 0:1].astype(jnp.int32) == i1, 1.0, 0.0).astype(BF16)
    out_ref[...] = jnp.dot(back, dc[...], preferred_element_type=F32).astype(BF16)


def tail(x, w, g, ln, parts):
    vm = pl.BlockSpec(memory_space=pltpu.VMEM)
    return pl.pallas_call(
        _tail, out_shape=(jax.ShapeDtypeStruct((S, E), BF16), jax.ShapeDtypeStruct((1, E), F32)), in_specs=[vm] * 8, out_specs=(vm, vm),
        scratch_shapes=[pltpu.VMEM((S, E), F32), pltpu.VMEM((S, E), BF16)],
        compiler_params=pltpu.CompilerParams(vmem_limit_bytes=LIMIT // 4), name="tail",
    )(x, w, g, ln, *parts)


def _dlogits(n, vb, hc_ref, rows_ref, emb_ref, part_ref, own_ref, sib_ref, all16, hc, ebuf, sbuf, bbuf, h_sem, e_sem, o_sem,
             x_sem, ss, rs, p_ss, p_rs):
    tp = lax.axis_index("tp")
    dp = lax.axis_index("dp")
    core = lax.rem(dp, 2)
    nblk = VH // vb
    steps = nblk // GROUP * TURN
    bar = pltpu.get_barrier_semaphore()

    def other(i):
        to = dp
        for bit in (1, 2, 4):
            to = to + bit * lax.rem(i // bit, 2) * (1 - 2 * lax.rem(dp // bit, 2))
        return {"tp": tp + i // NSEQ * (1 - 2 * tp), "dp": to}

    @pl.loop(*OTHERS)
    def _(i):
        pl.semaphore_signal(bar, inc=1, device_id=other(i), device_id_type=MESH)

    def place(i):
        q, k = i // TURN, lax.rem(i, TURN)
        extra = k // GROUP
        return extra, pl.multiple_of((q * GROUP + k - extra) * vb, vb)

    def row_of(i):
        extra, row = place(i)
        return pl.multiple_of((core + extra * (1 - 2 * core)) * VH + row, vb)

    def emb_copy(i):
        slot = lax.rem(i, 2)
        return pltpu.make_async_copy(emb_ref.at[pl.ds(row_of(i), vb)], ebuf.at[slot], e_sem.at[slot])

    def own_copy(i):
        slot = lax.rem(i, 2)
        return pltpu.make_async_copy(bbuf.at[slot], own_ref.at[pl.ds(place(i)[1], vb)], o_sem.at[slot])

    def extra_copy(i):
        slot = lax.rem(i, SLOTS)
        return pltpu.make_async_copy(sbuf.at[slot], sib_ref.at[pl.ds(place(i)[1], vb)], x_sem.at[slot])

    def send_copy(i):
        slot = lax.rem(i, SLOTS)
        return _remote(sbuf.at[slot], sib_ref.at[pl.ds(place(i)[1], vb)], ss.at[slot],
                       rs.at[i // TURN * SENT + lax.rem(i, TURN)], _dev(tp, dp, 0, 1))

    def free(i):
        @pl.when(lax.rem(i, TURN) < SENT)
        def _():
            send_copy(i).wait_send()

        @pl.when(lax.rem(i, TURN) == GROUP)
        def _():
            extra_copy(i).wait()

    h_copy = pltpu.make_async_copy(hc_ref.at[pl.ds(0, n)], hc, h_sem)
    h_copy.start()
    emb_copy(0).start()
    me = tp * 8 + dp
    all16[me] = part_ref[...]
    pl.semaphore_wait(bar, 15)

    def part_copy(i):
        return _remote(part_ref, all16.at[me], p_ss.at[i], p_rs.at[i], other(i))

    @pl.loop(*OTHERS)
    def _(i):
        part_copy(i).start()

    h_copy.wait()
    shift, coef_b = rows_ref[2:3, :n], rows_ref[3:4, :n]
    sub = lax.broadcasted_iota(jnp.int32, (vb, n), 0)

    @pl.loop(0, steps)
    def _(i):
        emb_copy(i).wait()

        @pl.when(i + 1 < steps)
        def _():
            emb_copy(i + 1).start()

        @pl.when((i > 1) & (lax.rem(i - 2, TURN) < GROUP))
        def _():
            own_copy(i - 2).wait()

        @pl.when(i >= SLOTS)
        def _():
            free(i - SLOTS)

        yy = rows_ref[0:1, :n].astype(jnp.int32) - (tp * VT + row_of(i))
        l = lax.dot_general(ebuf[lax.rem(i, 2)], hc[...], NT, preferred_element_type=F32)
        p = jnp.exp2(l * LOG2E - shift)
        p = jnp.where(sub == yy, p - coef_b, p)
        sbuf[lax.rem(i, SLOTS)] = p
        bbuf[lax.rem(i, 2)] = p.astype(BF16)

        @pl.when(lax.rem(i, TURN) < SENT)
        def _():
            send_copy(i).start()

        @pl.when(lax.rem(i, TURN) < GROUP)
        def _():
            own_copy(i).start()

        @pl.when(lax.rem(i, TURN) == GROUP)
        def _():
            extra_copy(i).start()

    own_copy(steps - 2).wait()
    for i in range(SLOTS):
        free(steps - SLOTS + i)

    @pl.loop(0, nblk // GROUP * SENT)
    def _(i):
        send_copy(i // SENT * TURN + lax.rem(i, SENT)).wait_recv()

    @pl.loop(*OTHERS)
    def _(i):
        part_copy(i).wait()


def dlogits(n, vb, cid, hc, rows, emb, part):
    dma = pltpu.SemaphoreType.DMA
    vm = pl.BlockSpec(memory_space=pltpu.VMEM)
    hbm = pl.BlockSpec(memory_space=pl.ANY)
    return pl.pallas_call(
        functools.partial(_dlogits, n, vb),
        out_shape=(jax.ShapeDtypeStruct((VH, n), BF16), jax.ShapeDtypeStruct((VH, n), F32), jax.ShapeDtypeStruct((16, 1, E), F32)),
        in_specs=[hbm, vm, hbm, vm], out_specs=(hbm, hbm, vm),
        scratch_shapes=[pltpu.VMEM((n, E), BF16), pltpu.VMEM((2, vb, E), BF16), pltpu.VMEM((SLOTS, vb, n), F32),
                        pltpu.VMEM((2, vb, n), BF16), dma, dma((2,)), dma((2,)), dma((SLOTS,)), dma((SLOTS,)),
                        dma((VH // vb // GROUP * SENT,)), dma((16,)), dma((16,))],
        compiler_params=pltpu.CompilerParams(collective_id=cid, has_side_effects=True, vmem_limit_bytes=LIMIT // 4 * 3),
        cost_estimate=pl.CostEstimate(flops=2 * VH * n * E, bytes_accessed=VH * E * 2 + 2 * VH * n * 4, transcendentals=0),
        name=f"dlogits{n}",
    )(hc, rows, emb, part)


def _demb(own_ref, sib_ref, hc_ref, out_ref):
    core = lax.rem(lax.axis_index("dp"), 2)
    out_ref[core] = jnp.dot(own_ref[...], hc_ref[...], preferred_element_type=F32)
    out_ref[1 - core] = jnp.dot(sib_ref[...].astype(BF16), hc_ref[...], preferred_element_type=F32)


def demb(n, vb, own, sib, hc):
    rows = pl.BlockSpec((vb, n), lambda i: (i, 0))
    return pl.pallas_call(
        _demb, grid=(VH // vb,),
        out_shape=jax.ShapeDtypeStruct((2, VH, E), F32),
        in_specs=[rows, rows, pl.BlockSpec((n, E), lambda i: (0, 0), pipeline_mode=pl.Buffered(1))],
        out_specs=pl.BlockSpec((2, vb, E), lambda i: (0, i, 0)),
        compiler_params=pltpu.CompilerParams(dimension_semantics=("arbitrary",), vmem_limit_bytes=LIMIT // 4 * 3),
        cost_estimate=pl.CostEstimate(flops=2 * VT * n * E, bytes_accessed=VT * E * 4 + VT * n * 3, transcendentals=0),
        name=f"demb{n}",
    )(own, sib, hc).reshape(VT, E)


def solution(mesh):
    swap_core = [(i, i ^ 1) for i in range(16)]
    swap_both = [(i, i ^ 9) for i in range(16)]

    def local_step(hidden, targets, weights, embedding, ln_scale):
        x = hidden[0]
        g = ln_scale[None, :]
        gath, stats, mine, other, part, cnt, which = front(x, weights, targets, g, embedding)
        hc, rows, loss = pack(cnt, stats, gath)

        def back_of(i, n, rows1, rows2):
            def run(hc, rows, emb, part, mine, other):
                own, sib, ln = dlogits(n, rows1, 1 + i, hc, rows, emb, part)
                mine, other, ln = lax.optimization_barrier((mine, other, ln))
                from_sib = lax.ppermute(other, ("tp", "dp"), swap_core)
                from_z = lax.ppermute(mine, "tp", [(0, 1), (1, 0)])
                from_both = lax.ppermute(other, ("tp", "dp"), swap_both)
                return demb(n, rows2, own, sib, hc), ln, from_sib, from_z, from_both
            return run

        branches = [back_of(i, *size) for i, size in enumerate(SIZES)]
        d_emb, ln, *theirs = lax.switch(which[0], branches, hc, rows, embedding, part, mine, other)
        d_hidden, dln = tail(x, weights, g, ln, (mine, *theirs))
        return loss[0, 0], d_hidden[None], d_emb, dln[0]

    return jax.shard_map(local_step, mesh=mesh,
                         in_specs=(P("dp", None, None), P("dp", None), P("dp", None), P("tp", None), P(None)),
                         out_specs=(P(), P("dp", None, None), P("tp", None), P(None)), check_vma=False)
```
